32 devices in a mesh: row: 8 (over z, y), col: 4 (over x, core).
Axes of the slice: x: 2, y: 2, z: 4, core: 2. Of those that a mesh axis runs over, the one named last changes fastest.
Arguments:
- fields: float32 [1, 4, 256, 256, 256], P(None, None, 'row', 'col'), may hold values from -6 to 6
- cotangent: float32 [1, 4, 256, 256, 256], P(None, None, 'row', 'col'), may hold values from -6 to 6
- spec_weights: float32 [2, 4, 4, 16, 16, 16], replicated, may hold values from -96 to 96
- point_weights: float32 [4, 4], replicated, may hold values from -3 to 3
- bias: float32 [4], replicated, may hold values from -3 to 3
Outputs:
- grad_fields: float32 [1, 4, 256, 256, 256], P(None, None, 'row', 'col')
- grad_spectral: float32 [2, 4, 4, 16, 16, 16], replicated
The draws below stay inside these ranges and needn't reach their ends.
All inputs are finite; a program needn't handle non-finite values.
Results may differ from the reference program's by a relative error of at most 0.00011.
Values sent between devices are 32-bit elements; how exact they have to be, the bound alone decides.
A program may use at most 128 MiB of HBM per device.

```python
import jax
import jax.numpy as jnp
from jax import lax

B = 1
C = 4
NX = 256
NY = 256
NZ = 256
MX = 16
MY = 16
MZ = 16


def block_levels(rng, shape, shards, smallest, top_value):
    factor_of, own = 1.0, jax.random.fold_in(rng, 6)
    for axis_at, parts in shards:
        draws = jnp.exp(jax.random.uniform(jax.random.fold_in(own, axis_at), (parts,), jnp.float32, smallest / len(shards), top_value / len(shards)))
        factor_of = factor_of * jnp.repeat(draws, shape[axis_at] // parts).reshape([-1 if axis == axis_at else 1 for axis in range(len(shape))])
    return factor_of


def gaussian(rng, extent, scale, most, cuts=(), kind=jnp.bfloat16):
    loudness = block_levels(rng, extent, cuts, -0.22, 0.18) if cuts else 1.0
    entries = jax.random.normal(rng, extent, jnp.float32) * scale * loudness
    return jnp.minimum(jnp.maximum(entries, -most), most).astype(kind)


def setup_inputs(seed: int = 0) -> dict:
    splits = jax.random.split(jax.random.key(seed), 6)
    return {
        "fields": gaussian(splits[0], (B, C, NY, NZ, NX), 1.0, 6.0, ((2, 8), (3, 4)), jnp.float32),
        "cotangent": gaussian(splits[1], (B, C, NY, NZ, NX), 1.0, 6.0, ((2, 8), (3, 4)), jnp.float32),
        "spec_weights": gaussian(splits[2], (2, C, C, MX, MY, MZ), ((NX * NY * NZ / (4.0 * C * MX * MY * MZ)) ** 0.5), 96.0, (), jnp.float32),
        "point_weights": gaussian(splits[3], (C, C), C ** -0.5, 3.0, (), jnp.float32),
        "bias": gaussian(splits[4], (C,), 0.5, 3.0, (), jnp.float32),
    }


def crop(spectrum):
    spectrum = spectrum[..., :MX]
    spectrum = jnp.concatenate([spectrum[..., :MY // 2, :, :], spectrum[..., NY - MY // 2:, :, :]], axis=-3)
    spectrum = jnp.concatenate([spectrum[..., :MZ // 2, :], spectrum[..., NZ - MZ // 2:, :]], axis=-2)
    return spectrum

def expand(modes):
    lead = modes.shape[:2]
    modes = jnp.pad(modes, [(0, 0), (0, 0), (0, 0), (0, 0), (0, NX // 2 + 1 - MX)])
    width_x = modes.shape[4]
    zeros_z = jnp.zeros(lead + (MY, NZ - MZ, width_x), modes.dtype)
    modes = jnp.concatenate([modes[..., :MZ // 2, :], zeros_z, modes[..., MZ // 2:, :]], axis=-2)
    zeros_y = jnp.zeros(lead + (NY - MY, NZ, width_x), modes.dtype)
    modes = jnp.concatenate([modes[..., :MY // 2, :, :], zeros_y, modes[..., MY // 2:, :, :]], axis=-3)
    return modes

def spectral(fields, spec_weights):
    spectrum = crop(jnp.fft.rfftn(fields, axes=(2, 3, 4)))
    weights = spec_weights[0] + 1j * spec_weights[1]
    mixed_modes = jnp.einsum('biqrp,iopqr->boqrp', spectrum, weights, precision=lax.Precision.HIGHEST)
    return jnp.fft.irfftn(expand(mixed_modes), s=(NY, NZ, NX), axes=(2, 3, 4))

def reference(fields, cotangent, spec_weights, point_weights, bias):

    def forward(field_in, weight_in):
        local_term = jnp.einsum('bcyzx,co->boyzx', field_in, point_weights, precision=lax.Precision.HIGHEST)
        pre_activation = spectral(field_in, weight_in) + local_term + bias[None, :, None, None, None]
        return jax.nn.gelu(pre_activation, approximate=False)
    output, pullback = jax.vjp(forward, fields, spec_weights)
    grad_fields, grad_spectral = pullback(cotangent.astype(output.dtype))
    return (grad_fields, grad_spectral)
```

```python
import functools
import math

import jax
import jax.numpy as jnp
import numpy as np
from jax import lax
from jax.experimental import pallas as pl
from jax.experimental.pallas import tpu as pltpu
from jax.sharding import PartitionSpec as P

f32 = jnp.float32
bf16 = jnp.bfloat16
MESH = pl.DeviceIdType.MESH
TILE = 512
ROWS = 8
LANES = 128


def split(value):
    high = value.astype(bf16)
    return high, (value - high.astype(f32)).astype(bf16)


def split_np(value):
    value = np.asarray(value, np.float32)
    high = value.astype(jnp.bfloat16)
    low = (value - high.astype(np.float32)).astype(jnp.bfloat16)
    return high, low


def signed(number):
    wave = np.arange(number)
    return np.where(wave < number // 2, wave, wave - number)


def x_tables(chans, length, modes, cells):
    angle = 2.0 * np.pi / length * ((np.arange(length)[:, None] * np.arange(modes)) % length)
    weight = np.where(np.arange(modes) == 0, 1.0, 2.0) / cells
    eye = np.eye(chans)
    first = np.stack([np.cos(angle), -np.sin(angle)], 1)
    wide = np.einsum("cd,xkp->cxkdp", eye, first).reshape(chans * length, -1)
    tall = np.einsum("cd,xkp->kcpdx", eye, first * weight).reshape(-1, chans * length)
    return np.concatenate(split_np(wide), 1), np.concatenate(split_np(tall), 0)


def yz_tables(ny, nz, my, mz, ty, ylines, zlines, nrow, ncol):
    ky, kz = np.repeat(signed(my), mz), np.tile(signed(mz), my)

    def turns(y, z):
        return ((np.outer(y, ky) % ny) / ny + (np.outer(z, kz) % nz) / nz) * 2.0 * np.pi

    angle = turns(np.repeat(np.arange(ty), zlines), np.tile(np.arange(zlines), ty))
    high, low = split_np(np.concatenate([np.cos(angle), np.sin(angle)], 1))
    device_y = np.repeat(np.arange(nrow) * ylines, ncol)
    device_z = np.tile(np.arange(ncol) * zlines, nrow)
    start = turns(device_y, device_z).T
    end = turns(device_y + ylines - ty, device_z).T
    step = turns(np.array([ty]), np.array([0])).T
    phase = np.concatenate(
        [np.cos(start), np.sin(start), np.cos(end), np.sin(end), np.cos(step), np.sin(step)], 1)
    return (np.concatenate([high.T, low.T], 1), np.concatenate([high, low], 1),
            phase.astype(np.float32))


def dot(a, b):
    return jnp.dot(a, b, preferred_element_type=f32)


def lane_ids(rows):
    return lax.broadcasted_iota(jnp.int32, (rows, LANES), 1)


def times_i(value):
    turned = pltpu.roll(value, LANES // 2, 1)
    return jnp.where(lane_ids(value.shape[0]) < LANES // 2, -turned, turned)


def analyse(xs, wt_v, an_v, acc, step_cos, step_sin):
    pairs = dot(xs[...], wt_v[...])
    part = jnp.concatenate(split(pairs[:, :LANES] + pairs[:, LANES:]), 1)
    both = dot(an_v[...], jnp.concatenate([part, part], 0))
    both = both[:, :LANES] + both[:, LANES:]
    modes = both.shape[0] // 2
    c, s = acc[0], acc[1]
    new_c = c * step_cos[...] + s * step_sin[...] + both[:modes]
    new_s = s * step_cos[...] - c * step_sin[...] + both[modes:]
    acc[0] = new_c
    acc[1] = new_s


def spectrum(acc, end_cos, end_sin):
    c, s = acc[0], acc[1]
    cosine = c * end_cos[...] - s * end_sin[...]
    sine = s * end_cos[...] + c * end_sin[...]
    return cosine - times_i(sine)


def mode_rhs(turn, rhs):
    modes = turn.shape[1]
    for k in range(2):
        high, low = split(turn[k])
        rhs[k * modes : (k + 1) * modes, :LANES] = high
        rhs[k * modes : (k + 1) * modes, LANES:] = low


def turn_on(turn, step_cos, step_sin):
    m, im = turn[0], turn[1]
    turn[0] = m * step_cos[...] + im * step_sin[...]
    turn[1] = im * step_cos[...] - m * step_sin[...]


def synthesise(sy_v, rhs, l_v, spec):
    pairs = dot(sy_v[...], jnp.concatenate([rhs[...], rhs[...]], 0))
    high, low = split(pairs[:, :LANES] + pairs[:, LANES:])
    spec[...] = dot(jnp.concatenate([high, low, high, low], 1), l_v[...])


def gelu_slope(v):
    arg = v * math.sqrt(0.5)
    gauss = jnp.exp2(arg * arg * (-1.0 / math.log(2.0)))
    return (0.5 * lax.erf(arg) + 0.5) + (v * (1.0 / math.sqrt(2.0 * math.pi))) * gauss


def fill_twice(src, dst, sems, at):
    rows, out = src.shape[0], []
    for k in range(2):
        out.append(pltpu.make_async_copy(src, dst.at[pl.ds(k * rows, rows)], sems.at[at + k]))
    return out


def fill_synthesis(src, dst, sems, at):
    rows, out = src.shape[0] // 2, []
    for k in range(4):
        out.append(pltpu.make_async_copy(
            src.at[pl.ds(k // 2 * rows, rows)], dst.at[pl.ds(k * rows, rows)], sems.at[at + k]))
    return out


def layer_kernel(dims, f_hbm, g_hbm, w_hbm, pw, bias, wt_hbm, l_hbm, an_hbm, sy_hbm, ph_ref,
                 loc_hbm, a_ref, u_ref, h_ref,
                 f_v, g_v, loc_v, w_v, wown, wt_v, l_v, an_v, sy_v, xs, spec, acc, turn, rhs,
                 phase, part, got1, got2, mg, ug, ag, hg,
                 f_sem, g_sem, out_sem, tab_sem,
                 s1, r1, sm, rm, su, ru, s2, r2, sa, ra, sh, rh):
    chans, mx, my, mz, ylines, zlines, nx, ty, count, cols, owners = dims
    modes = my * mz
    steps = ylines // ty
    me = lax.axis_index("row") * cols + lax.axis_index("col")

    def device(t):
        return {"row": t // cols, "col": lax.rem(t, cols)}

    barrier = pltpu.get_barrier_semaphore()

    def greet(k, carry):
        pl.semaphore_signal(barrier, inc=1, device_id=device(lax.rem(me + k, count)), device_id_type=MESH)
        return carry

    lax.fori_loop(1, count, greet, 0)

    q = jnp.minimum(me, owners - 1) * ROWS // mz
    r0 = pl.multiple_of(lax.rem(jnp.minimum(me, owners - 1) * ROWS, mz), ROWS)
    q8 = pl.multiple_of(q // 8 * 8, 8)

    def tile_copy(src, dst, sem, j):
        rows = pl.ds(j * ty, ty)
        return pltpu.make_async_copy(src.at[0, :, rows], dst.at[:, rows], sem.at[j])

    wt_copies = fill_twice(wt_hbm, wt_v, tab_sem, 0)
    l_copies = fill_synthesis(l_hbm, l_v, tab_sem, 2)
    an_copy = pltpu.make_async_copy(an_hbm, an_v, tab_sem.at[6])
    sy_copy = pltpu.make_async_copy(sy_hbm, sy_v, tab_sem.at[7])
    w_copy = pltpu.make_async_copy(w_hbm.at[:, pl.ds(q8, 8), :], w_v, tab_sem.at[8])
    for copy in wt_copies:
        copy.start()
    tile_copy(f_hbm, f_v, f_sem, 0).start()
    an_copy.start()
    for j in range(1, steps):
        tile_copy(f_hbm, f_v, f_sem, j).start()
    w_copy.start()
    sy_copy.start()
    for copy in l_copies:
        copy.start()
    for j in range(steps):
        tile_copy(g_hbm, g_v, g_sem, j).start()

    place = lax.broadcasted_iota(jnp.int32, (modes, count), 1) == me
    for k in range(4):
        column = jnp.sum(jnp.where(place, ph_ref[:, k * count : (k + 1) * count], 0.0), axis=1, keepdims=True)
        phase[k] = jnp.broadcast_to(column, (modes, LANES))
    for k in range(2):
        phase[4 + k] = jnp.broadcast_to(ph_ref[:, 4 * count + k : 4 * count + k + 1], (modes, LANES))
    start_cos, start_sin, end_cos, end_sin, step_cos, step_sin = [phase.at[k] for k in range(6)]
    acc[...] = jnp.zeros_like(acc)

    for copy in wt_copies:
        copy.wait()
    an_copy.wait()

    def first(j, carry):
        tile_copy(f_hbm, f_v, f_sem, j).wait()

        def cut(k, carry):
            rows = pl.ds(pl.multiple_of(k * zlines, zlines), zlines)
            for c in range(chans):
                high, low = split(f_v[c, j * ty + k])
                xs[rows, c * nx : (c + 1) * nx] = high
                xs[rows, (chans + c) * nx : (chans + c + 1) * nx] = low
            return carry

        lax.fori_loop(0, ty, cut, 0)
        analyse(xs, wt_v, an_v, acc, step_cos, step_sin)
        return carry

    lax.fori_loop(0, steps, first, 0)
    part[0] = spectrum(acc, end_cos, end_sin).reshape(owners, ROWS, LANES)
    pl.semaphore_wait(barrier, count - 1)

    def piece(src, dst, send, recv, k, arriving, scatter):
        t = lax.rem(me + k, count)
        slot = t if arriving else me
        return pltpu.make_async_remote_copy(
            src_ref=src.at[t if scatter else me], dst_ref=dst.at[slot], send_sem=send.at[t],
            recv_sem=recv.at[slot], device_id=device(t), device_id_type=MESH)

    def each(action):
        def body(k, carry):
            action(k)
            return carry
        lax.fori_loop(1, count, body, 0)

    def owned(k, action):
        if owners == count:
            action()
        else:
            pl.when(lax.rem(me + k, count) < owners)(action)

    def owner(action):
        if owners == count:
            action()
        else:
            pl.when(me < owners)(action)

    def scatter_start(src, dst, send, recv):
        each(lambda k: owned(k, lambda: piece(src, dst, send, recv, k, False, True).start()))

    def scatter_sent(src, dst, send, recv):
        each(lambda k: owned(k, lambda: piece(src, dst, send, recv, k, False, True).wait_send()))

    def scatter_sum(src, dst, send, recv):
        each(lambda k: piece(src, dst, send, recv, k, True, False).wait_recv())
        dst[pl.ds(me, 1)] = src[pl.ds(me, 1)]
        return jnp.sum(dst[...], axis=0)

    def gather_start(ref, send, recv):
        each(lambda k: piece(ref, ref, send, recv, k, False, False).start())

    def gather_wait(ref, send, recv):
        each(lambda k: owned(k, lambda: piece(ref, ref, send, recv, k, True, False).wait_recv()))

    def gather_sent(ref, send, recv):
        owner(lambda: each(lambda k: piece(ref, ref, send, recv, k, False, False).wait_send()))

    scatter_start(part.at[0], got1, s1, r1)

    w_copy.wait()
    rows_w = chans * mx * 2
    for b in range(w_v.shape[0] // rows_w):
        wown[b] = w_v[rows_w * b : rows_w * (b + 1), q - q8, :].T

    step = 16
    per = zlines // step

    def local(k, carry):
        y, z = k // per, k % per
        zs = pl.ds(pl.multiple_of(z * step, step), step)
        fields = [f_v[i, y, zs, :] for i in range(chans)]
        for o in range(chans):
            total = fields[0] * pw[0, o] + bias[o]
            for i in range(1, chans):
                total += fields[i] * pw[i, o]
            loc_v[o, y, zs, :] = total
        return carry

    lax.fori_loop(0, ylines * per, local, 0)

    lane = lane_ids(ROWS)
    low_half = lane < LANES // 2
    group = lane % mx

    def take(value, index):
        return jnp.take_along_axis(value, index, axis=1)

    def weights():
        return [wown[b, pl.ds(r0, ROWS), :] for b in range(2 * chans // 2)]

    def mix_first():
        u = scatter_sum(part.at[0], got1, s1, r1)
        ug[pl.ds(me, 1)] = u[None]
        w = weights()
        real = imag = 0.0
        for pair in range(2):
            index = (2 * pair + lane // (LANES // 2)) * mx + group
            ur, ui = take(u, index), take(u, index + LANES // 2)
            wr, wi = w[pair], w[2 + pair]
            real += wr * ur - wi * ui
            imag += wr * ui + wi * ur
        real += pltpu.roll(real, LANES // 2, 1)
        imag += pltpu.roll(imag, LANES // 2, 1)
        mg[pl.ds(me, 1)] = jnp.where(low_half, real, imag)[None]
        gather_start(mg, sm, rm)
        gather_start(ug, su, ru)

    owner(mix_first)
    sy_copy.wait()
    for copy in l_copies:
        copy.wait()
    gather_wait(mg, sm, rm)

    def load_turn(ref):
        m = ref[...].reshape(modes, LANES)
        im = times_i(m)
        turn[0] = m * start_cos[...] + im * start_sin[...]
        turn[1] = im * start_cos[...] - m * start_sin[...]

    load_turn(mg)
    acc[...] = jnp.zeros_like(acc)

    def second(j, carry):
        mode_rhs(turn, rhs)
        synthesise(sy_v, rhs, l_v, spec)
        turn_on(turn, step_cos, step_sin)
        tile_copy(g_hbm, g_v, g_sem, j).wait()

        def cells(k, carry):
            y, z = j * ty + k // per, k % per
            zs = pl.ds(pl.multiple_of(z * step, step), step)
            rows = pl.ds(pl.multiple_of(k * step, step), step)
            for o in range(chans):
                pre = spec[rows, o * nx : (o + 1) * nx] + loc_v[o, y, zs, :]
                up = g_v[o, y, zs, :] * gelu_slope(pre)
                g_v[o, y, zs, :] = up
                high, low = split(up)
                xs[rows, o * nx : (o + 1) * nx] = high
                xs[rows, (chans + o) * nx : (chans + o + 1) * nx] = low
            return carry

        lax.fori_loop(0, ty * per, cells, 0)
        analyse(xs, wt_v, an_v, acc, step_cos, step_sin)
        return carry

    lax.fori_loop(0, steps, second, 0)
    part[1] = spectrum(acc, end_cos, end_sin).reshape(owners, ROWS, LANES)
    scatter_start(part.at[1], got2, s2, r2)

    def out_copy(j):
        rows = pl.ds(j * ty, ty)
        return pltpu.make_async_copy(loc_v.at[:, rows], loc_hbm.at[0, :, rows], out_sem.at[j])

    def back(j, carry):
        def cells(k, carry):
            y, z = j * ty + k // per, k % per
            zs = pl.ds(pl.multiple_of(z * step, step), step)
            ups = [g_v[o, y, zs, :] for o in range(chans)]
            for i in range(chans):
                total = ups[0] * pw[i, 0]
                for o in range(1, chans):
                    total += ups[o] * pw[i, o]
                loc_v[i, y, zs, :] = total
            return carry

        lax.fori_loop(0, ty * per, cells, 0)
        out_copy(j).start()
        return carry

    lax.fori_loop(0, steps, back, 0)

    def mix_second():
        h = scatter_sum(part.at[1], got2, s2, r2)
        hg[pl.ds(me, 1)] = h[None]
        w = weights()
        other = pltpu.roll(h, LANES // 2, 1)
        hr, hi = jnp.where(low_half, h, other), jnp.where(low_half, other, h)
        result = jnp.zeros_like(h)
        for pair in range(2):
            wr, wi = w[pair], w[2 + pair]
            for k, value in enumerate((wr * hr + wi * hi, wr * hi - wi * hr)):
                total = value
                for o in range(1, chans):
                    total += pltpu.roll(value, o * mx, 1)
                chan = lane // mx % chans
                index = chan % 2 * (LANES // 2) + (chans - 1) * mx + group
                here = (lane // (LANES // 2) == k) & (chan // 2 == pair)
                result = jnp.where(here, take(total, index), result)
        ag[pl.ds(me, 1)] = result[None]
        gather_start(ag, sa, ra)
        gather_start(hg, sh, rh)

    owner(mix_second)
    gather_wait(ug, su, ru)
    u_ref[...] = ug[...].reshape(modes, LANES)
    scatter_sent(part.at[0], got1, s1, r1)
    gather_sent(mg, sm, rm)
    gather_sent(ug, su, ru)
    scatter_sent(part.at[1], got2, s2, r2)
    gather_wait(ag, sa, ra)
    a_ref[...] = ag[...].reshape(modes, LANES)
    gather_wait(hg, sh, rh)
    h_ref[...] = hg[...].reshape(modes, LANES)
    gather_sent(ag, sa, ra)
    gather_sent(hg, sh, rh)
    for j in range(steps):
        out_copy(j).wait()


def gradient_kernel(dims, cells_all, a_ref, u_ref, h_ref, ph_ref, loc_ref, l_hbm, sy_ref,
                    o_ref, gs_ref, l_v, spec, turn, rhs, phase, ut, ht, sems):
    chans, mx, my, mz, ylines, zlines, nx, ty, count, cols, owners = dims
    modes = my * mz
    steps = ylines // ty
    j = pl.program_id(0)
    me = lax.axis_index("row") * cols + lax.axis_index("col")

    @pl.when(j == 0)
    def _():
        copies = fill_synthesis(l_hbm, l_v, sems, 0)
        for copy in copies:
            copy.start()
        place = lax.broadcasted_iota(jnp.int32, (modes, count), 1) == me
        found = []
        for k in range(2):
            column = jnp.sum(jnp.where(place, ph_ref[:, k * count : (k + 1) * count], 0.0), axis=1, keepdims=True)
            found.append(jnp.broadcast_to(column, (modes, LANES)))
            phase[k] = jnp.broadcast_to(ph_ref[:, 4 * count + k : 4 * count + k + 1], (modes, LANES))
        m = a_ref[...]
        im = times_i(m)
        turn[0] = m * found[0] + im * found[1]
        turn[1] = im * found[0] - m * found[1]
        ut[...] = u_ref[...].T
        ht[...] = h_ref[...].T
        for copy in copies:
            copy.wait()

    mode_rhs(turn, rhs)
    synthesise(sy_ref, rhs, l_v, spec)
    turn_on(turn, phase.at[0], phase.at[1])
    step = 16
    per = zlines // step

    def cells(k, carry):
        y, z = k // per, k % per
        zs = pl.ds(pl.multiple_of(z * step, step), step)
        rows = pl.ds(pl.multiple_of(k * step, step), step)
        for i in range(chans):
            o_ref[0, i, y, zs, :] = spec[rows, i * nx : (i + 1) * nx] + loc_ref[0, i, y, zs, :]
        return carry

    lax.fori_loop(0, ty * per, cells, 0)

    blocks = 2 * chans * chans // steps
    wave = lax.broadcasted_iota(jnp.int32, (mx, modes), 0)
    factor = jnp.where(wave == 0, 1.0 / cells_all, 2.0 / cells_all).astype(f32)

    def weight(b, carry):
        at = j * blocks + b
        k, i, o = at // (chans * chans), at // chans % chans, at % chans

        def rows_of(ref, kind, c):
            return ref[pl.ds(pl.multiple_of((kind * chans + c) * mx, mx), mx), :]

        ur, ui, hr, hi = rows_of(ut, 0, i), rows_of(ut, 1, i), rows_of(ht, 0, o), rows_of(ht, 1, o)
        value = jnp.where(k == 0, ur * hr + ui * hi, ur * hi - ui * hr) * factor
        out = pl.ds(pl.multiple_of(b * mx, mx), mx)
        for q in range(my):
            lo = q * mz // LANES * LANES
            shift = q * mz - lo
            half = value[:, lo : lo + LANES]
            moved = pltpu.roll(half, LANES - shift, 1) if shift else half
            gs_ref[out, q, :] = moved[:, :mz]
        return carry

    lax.fori_loop(0, blocks, weight, 0)


def solution(mesh):
    nrow, ncol = mesh.shape["row"], mesh.shape["col"]
    count = nrow * ncol

    def per_device(fields, cotangent, spec_weights, point_weights, bias):
        _, chans, ylines, zlines, nx = fields.shape
        _, _, _, mx, my, mz = spec_weights.shape
        ny, nz = ylines * nrow, zlines * ncol
        modes = my * mz
        owners = min(count, modes // ROWS)
        cells_all = float(nx * ny * nz)
        ty = max(1, min(ylines, TILE // zlines))
        steps = ylines // ty
        tile = ty * zlines
        dims = (chans, mx, my, mz, ylines, zlines, nx, ty, count, ncol, owners)
        wt_tab, l_tab = x_tables(chans, nx, mx, cells_all)
        an_tab, sy_tab, ph_tab = yz_tables(ny, nz, my, mz, ty, ylines, zlines, nrow, ncol)
        flat = (2 * chans * chans * mx, my, mz)
        weights = spec_weights.reshape(flat)

        anyspace = pl.BlockSpec(memory_space=pl.ANY)
        vmem = pl.BlockSpec(memory_space=pltpu.VMEM)
        smem = pl.BlockSpec(memory_space=pltpu.SMEM)
        field_shape = jax.ShapeDtypeStruct(fields.shape, f32)
        mode_shape = jax.ShapeDtypeStruct((modes, LANES), f32)
        block = fields.shape[1:]
        gathered = pltpu.VMEM((owners, ROWS, LANES), f32)
        arrived = pltpu.VMEM((count, ROWS, LANES), f32)
        tables = [
            pltpu.VMEM((2 * chans * nx, 2 * LANES), bf16),
            pltpu.VMEM((4 * LANES, chans * nx), bf16),
            pltpu.VMEM((2 * modes, 2 * tile), bf16),
            pltpu.VMEM((tile, 4 * modes), bf16),
        ]
        spec_v = pltpu.VMEM((tile, chans * nx), f32)
        turn_v = pltpu.VMEM((2, modes, LANES), f32)
        rhs_v = pltpu.VMEM((2 * modes, 2 * LANES), bf16)
        dma = pltpu.SemaphoreType.DMA

        local, adjoint, spectrum_u, spectrum_h = pl.pallas_call(
            functools.partial(layer_kernel, dims),
            out_shape=(field_shape, mode_shape, mode_shape, mode_shape),
            in_specs=[anyspace, anyspace, anyspace, smem, smem, anyspace, anyspace, anyspace, anyspace, vmem],
            out_specs=(anyspace, vmem, vmem, vmem),
            scratch_shapes=[
                pltpu.VMEM(block, f32), pltpu.VMEM(block, f32), pltpu.VMEM(block, f32),
                pltpu.VMEM((flat[0], 8, mz), f32),
                pltpu.VMEM((flat[0] // LANES, mz, LANES), f32),
                *tables,
                pltpu.VMEM((tile, 2 * chans * nx), bf16), spec_v,
                pltpu.VMEM((2, modes, LANES), f32), turn_v, rhs_v,
                pltpu.VMEM((6, modes, LANES), f32),
                pltpu.VMEM((2, owners, ROWS, LANES), f32),
                arrived, arrived, gathered, gathered, gathered, gathered,
                dma((steps,)), dma((steps,)), dma((steps,)), dma((9,)),
                *[dma((count,))] * 12,
            ],
            compiler_params=pltpu.CompilerParams(
                collective_id=0, has_side_effects=True, vmem_limit_bytes=60 * 1024 * 1024),
            name="layer",
        )(fields, cotangent, weights, point_weights, bias, wt_tab, l_tab, an_tab, sy_tab, ph_tab)

        def keep(shape):
            return pl.BlockSpec(shape, lambda j: (0,) * len(shape))

        cells = pl.BlockSpec((1, chans, ty, zlines, nx), lambda j: (0, 0, j, 0, 0))
        mode = keep((modes, LANES))
        grad_fields, grad_spectral = pl.pallas_call(
            functools.partial(gradient_kernel, dims, cells_all),
            grid=(steps,),
            out_shape=(field_shape, jax.ShapeDtypeStruct(flat, f32)),
            in_specs=[mode, mode, mode, keep(ph_tab.shape), cells, anyspace, keep(sy_tab.shape)],
            out_specs=(cells, pl.BlockSpec((flat[0] // steps, my, mz), lambda j: (j, 0, 0))),
            scratch_shapes=[
                tables[1], spec_v, turn_v, rhs_v, pltpu.VMEM((2, modes, LANES), f32),
                pltpu.VMEM((LANES, modes), f32), pltpu.VMEM((LANES, modes), f32), dma((4,)),
            ],
            compiler_params=pltpu.CompilerParams(
                dimension_semantics=("arbitrary",), vmem_limit_bytes=56 * 1024 * 1024),
            name="gradients",
        )(adjoint, spectrum_u, spectrum_h, ph_tab, local, l_tab, sy_tab)
        return grad_fields, grad_spectral.reshape(spec_weights.shape)

    placed = (P(None, None, "row", "col", None), P(None, None, "row", "col", None), P(), P(), P())
    return jax.shard_map(
        per_device,
        mesh=mesh,
        in_specs=placed,
        out_specs=(P(None, None, "row", "col", None), P()),
        check_vma=False,
    )
```

```python
import functools
import math

import jax
import jax.numpy as jnp
import numpy as np
from jax import lax
from jax.experimental import pallas as pl
from jax.experimental.pallas import tpu as pltpu
from jax.sharding import PartitionSpec as P

f32 = jnp.float32
bf16 = jnp.bfloat16
MESH = pl.DeviceIdType.MESH
TILE = 512
ROWS = 8
LANES = 128


def split(value):
    high = value.astype(bf16)
    return high, (value - high.astype(f32)).astype(bf16)


def split_np(value):
    value = np.asarray(value, np.float32)
    high = value.astype(jnp.bfloat16)
    low = (value - high.astype(np.float32)).astype(jnp.bfloat16)
    return high, low


def signed(number):
    wave = np.arange(number)
    return np.where(wave < number // 2, wave, wave - number)


def x_tables(chans, length, modes, cells):
    angle = 2.0 * np.pi / length * ((np.arange(length)[:, None] * np.arange(modes)) % length)
    weight = np.where(np.arange(modes) == 0, 1.0, 2.0) / cells
    first = np.stack([np.cos(angle), -np.sin(angle)], 1)
    eye = np.eye(chans).reshape(chans, chans // 2, 2)
    wide = np.einsum("cgd,xkp->cxgkdp", eye, first).reshape(chans, 1, length, -1)
    wide = np.repeat(wide, 2, 1).reshape(2 * chans * length, -1)
    tall = np.einsum("de,xkp->kdpex", np.eye(2), first * weight).reshape(-1, 2 * length)
    high, low = split_np(tall)
    return np.concatenate(split_np(wide), 1), np.concatenate([high, high, low, 0 * low], 0)


def yz_tables(ny, nz, my, mz, ty, ylines, zlines, nrow, ncol):
    ky, kz = np.repeat(signed(my), mz), np.tile(signed(mz), my)

    def turns(y, z):
        return ((np.outer(y, ky) % ny) / ny + (np.outer(z, kz) % nz) / nz) * 2.0 * np.pi

    angle = turns(np.repeat(np.arange(ty), zlines), np.tile(np.arange(zlines), ty))
    high, low = split_np(np.concatenate([np.cos(angle), np.sin(angle)], 1))
    device_y = np.repeat(np.arange(nrow) * ylines, ncol)
    device_z = np.tile(np.arange(ncol) * zlines, nrow)
    start = turns(device_y, device_z).T
    end = turns(device_y + ylines - ty, device_z).T
    step = turns(np.array([ty]), np.array([0])).T
    phase = np.concatenate(
        [np.cos(start), np.sin(start), np.cos(end), np.sin(end), np.cos(step), np.sin(step)], 1)
    return (np.concatenate([high.T, low.T], 1), np.concatenate([high, low], 1),
            phase.astype(np.float32))


def dot(a, b):
    return jnp.dot(a, b, preferred_element_type=f32)


def lane_ids(rows):
    return lax.broadcasted_iota(jnp.int32, (rows, LANES), 1)


def times_i(value):
    quarter = LANES // 4
    real = lane_ids(value.shape[0]) % (LANES // 2) < quarter
    return jnp.where(real, -pltpu.roll(value, LANES - quarter, 1), pltpu.roll(value, quarter, 1))


def along_x(value, c, xs, wt_v):
    width = value.shape[1]
    at = 2 * c * width
    high, low = split(value)
    xs[:, at : at + width] = high
    xs[:, at + width : at + 2 * width] = low
    return dot(xs[:, at : at + 2 * width], wt_v[at : at + 2 * width, :])


def analyse(pairs, an_v, acc, step_cos, step_sin):
    part = jnp.concatenate(split(pairs[:, :LANES] + pairs[:, LANES:]), 1)
    both = dot(an_v[...], jnp.concatenate([part, part], 0))
    both = both[:, :LANES] + both[:, LANES:]
    modes = both.shape[0] // 2
    c, s = acc[0], acc[1]
    new_c = c * step_cos[...] + s * step_sin[...] + both[:modes]
    new_s = s * step_cos[...] - c * step_sin[...] + both[modes:]
    acc[0] = new_c
    acc[1] = new_s


def spectrum(acc, end_cos, end_sin):
    c, s = acc[0], acc[1]
    cosine = c * end_cos[...] - s * end_sin[...]
    sine = s * end_cos[...] + c * end_sin[...]
    return cosine - times_i(sine)


def mode_rhs(turn, rhs):
    modes = turn.shape[1]
    for k in range(2):
        high, low = split(turn[k])
        rhs[k * modes : (k + 1) * modes, :LANES] = high
        rhs[k * modes : (k + 1) * modes, LANES:] = low


def turn_on(turn, step_cos, step_sin):
    m, im = turn[0], turn[1]
    turn[0] = m * step_cos[...] + im * step_sin[...]
    turn[1] = im * step_cos[...] - m * step_sin[...]


def synthesise(sy_v, rhs, lhs):
    pairs = dot(sy_v[...], jnp.concatenate([rhs[...], rhs[...]], 0))
    value = pairs[:, :LANES] + pairs[:, LANES:]
    other = pltpu.roll(value, LANES // 2, 1)
    lower = lane_ids(value.shape[0]) < LANES // 2
    for pair in range(2):
        twice = jnp.where(lower, value, other) if pair == 0 else jnp.where(lower, other, value)
        high = twice.astype(bf16)
        wide = high.astype(f32)
        lhs[pair, :, :LANES] = jnp.where(lower, wide, twice - wide).astype(bf16)
        lhs[pair, :, LANES:] = high


def back_to_x(lhs, l_v, c):
    nx = l_v.shape[1] // 2
    return dot(lhs[c // 2], l_v[:, c % 2 * nx : (c % 2 + 1) * nx])


def gelu_slope(v):
    arg = v * math.sqrt(0.5)
    gauss = jnp.exp2(arg * arg * (-1.0 / math.log(2.0)))
    return (0.5 * lax.erf(arg) + 0.5) + (v * (1.0 / math.sqrt(2.0 * math.pi))) * gauss


def layer_kernel(dims, f_hbm, g_hbm, w_hbm, pw, bias, wt_hbm, l_hbm, an_hbm, sy_hbm, ph_ref,
                 loc_hbm, a_ref, u_ref, h_ref,
                 f_v, g_v, loc_v, w_v, wown, wt_v, l_v, an_v, sy_v, xs, lhs, acc, turn, rhs,
                 phase, part, got1, got2, mg, ug, ag, hg,
                 f_sem, g_sem, out_sem, tab_sem,
                 s1, r1, sm, rm, su, ru, s2, r2, sa, ra, sh, rh):
    chans, mx, my, mz, ylines, zlines, nx, ty, count, cols, owners = dims
    modes = my * mz
    steps = ylines // ty
    tile = ty * zlines
    me = lax.axis_index("row") * cols + lax.axis_index("col")

    def device(t):
        return {"row": t // cols, "col": lax.rem(t, cols)}

    barrier = pltpu.get_barrier_semaphore()

    def greet(k, carry):
        pl.semaphore_signal(barrier, inc=1, device_id=device(lax.rem(me + k, count)), device_id_type=MESH)
        return carry

    lax.fori_loop(1, count, greet, 0)

    q = jnp.minimum(me, owners - 1) * ROWS // mz
    r0 = pl.multiple_of(lax.rem(jnp.minimum(me, owners - 1) * ROWS, mz), ROWS)
    q8 = pl.multiple_of(q // 8 * 8, 8)

    def tile_copy(src, dst, sem, j):
        rows = pl.ds(j * ty, ty)
        return pltpu.make_async_copy(src.at[0, :, rows], dst.at[:, rows], sem.at[j])

    wt_copy = pltpu.make_async_copy(wt_hbm, wt_v, tab_sem.at[0])
    l_copy = pltpu.make_async_copy(l_hbm, l_v, tab_sem.at[1])
    an_copy = pltpu.make_async_copy(an_hbm, an_v, tab_sem.at[2])
    sy_copy = pltpu.make_async_copy(sy_hbm, sy_v, tab_sem.at[3])
    w_copy = pltpu.make_async_copy(w_hbm.at[:, pl.ds(q8, 8), :], w_v, tab_sem.at[4])
    wt_copy.start()
    tile_copy(f_hbm, f_v, f_sem, 0).start()
    an_copy.start()
    for j in range(1, steps):
        tile_copy(f_hbm, f_v, f_sem, j).start()
    w_copy.start()
    sy_copy.start()
    l_copy.start()
    for j in range(steps):
        tile_copy(g_hbm, g_v, g_sem, j).start()

    place = lax.broadcasted_iota(jnp.int32, (modes, count), 1) == me
    for k in range(4):
        column = jnp.sum(jnp.where(place, ph_ref[:, k * count : (k + 1) * count], 0.0), axis=1, keepdims=True)
        phase[k] = jnp.broadcast_to(column, (modes, LANES))
    for k in range(2):
        phase[4 + k] = jnp.broadcast_to(ph_ref[:, 4 * count + k : 4 * count + k + 1], (modes, LANES))
    start_cos, start_sin, end_cos, end_sin, step_cos, step_sin = [phase.at[k] for k in range(6)]
    acc[...] = jnp.zeros_like(acc)

    wt_copy.wait()
    an_copy.wait()

    def first(j, carry):
        tile_copy(f_hbm, f_v, f_sem, j).wait()

        pairs = 0.0
        for c in range(chans):
            pairs += along_x(f_v[c, pl.ds(j * ty, ty)].reshape(tile, nx), c, xs, wt_v)
        analyse(pairs, an_v, acc, step_cos, step_sin)
        return carry

    lax.fori_loop(0, steps, first, 0)
    part[0] = spectrum(acc, end_cos, end_sin).reshape(owners, ROWS, LANES)
    pl.semaphore_wait(barrier, count - 1)

    def piece(src, dst, send, recv, k, arriving, scatter):
        t = lax.rem(me + k, count)
        slot = t if arriving else me
        return pltpu.make_async_remote_copy(
            src_ref=src.at[t if scatter else me], dst_ref=dst.at[slot], send_sem=send.at[t],
            recv_sem=recv.at[slot], device_id=device(t), device_id_type=MESH)

    def each(action):
        def body(k, carry):
            action(k)
            return carry
        lax.fori_loop(1, count, body, 0)

    def owned(k, action):
        if owners == count:
            action()
        else:
            pl.when(lax.rem(me + k, count) < owners)(action)

    def owner(action):
        if owners == count:
            action()
        else:
            pl.when(me < owners)(action)

    def scatter_start(src, dst, send, recv):
        each(lambda k: owned(k, lambda: piece(src, dst, send, recv, k, False, True).start()))

    def scatter_sent(src, dst, send, recv):
        each(lambda k: owned(k, lambda: piece(src, dst, send, recv, k, False, True).wait_send()))

    def scatter_sum(src, dst, send, recv):
        each(lambda k: piece(src, dst, send, recv, k, True, False).wait_recv())
        dst[pl.ds(me, 1)] = src[pl.ds(me, 1)]
        return jnp.sum(dst[...], axis=0)

    def gather_start(ref, send, recv):
        each(lambda k: piece(ref, ref, send, recv, k, False, False).start())

    def gather_wait(ref, send, recv):
        each(lambda k: owned(k, lambda: piece(ref, ref, send, recv, k, True, False).wait_recv()))

    def gather_sent(ref, send, recv):
        owner(lambda: each(lambda k: piece(ref, ref, send, recv, k, False, False).wait_send()))

    scatter_start(part.at[0], got1, s1, r1)

    w_copy.wait()
    rows_w = chans * mx * 2
    for b in range(w_v.shape[0] // rows_w):
        wown[b] = w_v[rows_w * b : rows_w * (b + 1), q - q8, :].T

    step = 16
    per = zlines // step

    def local(k, carry):
        y, z = k // per, k % per
        zs = pl.ds(pl.multiple_of(z * step, step), step)
        fields = [f_v[i, y, zs, :] for i in range(chans)]
        for o in range(chans):
            total = fields[0] * pw[0, o] + bias[o]
            for i in range(1, chans):
                total += fields[i] * pw[i, o]
            loc_v[o, y, zs, :] = total
        return carry

    lax.fori_loop(0, ylines * per, local, 0)

    lane = lane_ids(ROWS)
    quarter = LANES // 4
    is_real = lane % (LANES // 2) < quarter
    wave = lane % mx

    def lane_of(kind, chan):
        return chan // 2 * (LANES // 2) + kind * quarter + chan % 2 * mx + wave

    def take(value, index):
        return jnp.take_along_axis(value, index, axis=1)

    def weights():
        return [wown[b, pl.ds(r0, ROWS), :] for b in range(2 * chans // 2)]

    def mix_first():
        u = scatter_sum(part.at[0], got1, s1, r1)
        ug[pl.ds(me, 1)] = u[None]
        w = weights()
        real = imag = 0.0
        for pair in range(2):
            chan = 2 * pair + lane // (LANES // 2)
            ur, ui = take(u, lane_of(0, chan)), take(u, lane_of(1, chan))
            wr, wi = w[pair], w[2 + pair]
            real += wr * ur - wi * ui
            imag += wr * ui + wi * ur
        real += pltpu.roll(real, LANES // 2, 1)
        imag += pltpu.roll(imag, LANES // 2, 1)
        source = lane // (LANES // 2) * quarter + lane % quarter
        mg[pl.ds(me, 1)] = jnp.where(is_real, take(real, source), take(imag, source))[None]
        gather_start(mg, sm, rm)
        gather_start(ug, su, ru)

    owner(mix_first)
    sy_copy.wait()
    l_copy.wait()
    gather_wait(mg, sm, rm)

    def load_turn(ref):
        m = ref[...].reshape(modes, LANES)
        im = times_i(m)
        turn[0] = m * start_cos[...] + im * start_sin[...]
        turn[1] = im * start_cos[...] - m * start_sin[...]

    load_turn(mg)
    acc[...] = jnp.zeros_like(acc)

    def second(j, carry):
        mode_rhs(turn, rhs)
        synthesise(sy_v, rhs, lhs)
        turn_on(turn, step_cos, step_sin)
        tile_copy(g_hbm, g_v, g_sem, j).wait()
        lines = pl.ds(j * ty, ty)
        pairs = 0.0
        for o in range(chans):
            pre = back_to_x(lhs, l_v, o) + loc_v[o, lines].reshape(tile, nx)
            up = g_v[o, lines].reshape(tile, nx) * gelu_slope(pre)
            g_v[o, lines] = up.reshape(ty, zlines, nx)
            pairs += along_x(up, o, xs, wt_v)
        analyse(pairs, an_v, acc, step_cos, step_sin)
        return carry

    lax.fori_loop(0, steps, second, 0)
    part[1] = spectrum(acc, end_cos, end_sin).reshape(owners, ROWS, LANES)
    scatter_start(part.at[1], got2, s2, r2)

    def out_copy(j):
        rows = pl.ds(j * ty, ty)
        return pltpu.make_async_copy(loc_v.at[:, rows], loc_hbm.at[0, :, rows], out_sem.at[j])

    def back(j, carry):
        def cells(k, carry):
            y, z = j * ty + k // per, k % per
            zs = pl.ds(pl.multiple_of(z * step, step), step)
            ups = [g_v[o, y, zs, :] for o in range(chans)]
            for i in range(chans):
                total = ups[0] * pw[i, 0]
                for o in range(1, chans):
                    total += ups[o] * pw[i, o]
                loc_v[i, y, zs, :] = total
            return carry

        lax.fori_loop(0, ty * per, cells, 0)
        out_copy(j).start()
        return carry

    lax.fori_loop(0, steps, back, 0)

    def mix_second():
        h = scatter_sum(part.at[1], got2, s2, r2)
        hg[pl.ds(me, 1)] = h[None]
        w = weights()
        chan = lane // mx % chans
        hr, hi = take(h, lane_of(0, chan)), take(h, lane_of(1, chan))
        result = jnp.zeros_like(h)
        for pair in range(2):
            wr, wi = w[pair], w[2 + pair]
            for k, value in enumerate((wr * hr + wi * hi, wr * hi - wi * hr)):
                total = value
                for o in range(1, chans):
                    total += pltpu.roll(value, o * mx, 1)
                index = lane % quarter // mx * (LANES // 2) + (chans - 1) * mx + wave
                here = (is_real if k == 0 else jnp.logical_not(is_real)) & (lane // (LANES // 2) == pair)
                result = jnp.where(here, take(total, index), result)
        ag[pl.ds(me, 1)] = result[None]
        gather_start(ag, sa, ra)
        gather_start(hg, sh, rh)

    owner(mix_second)
    gather_wait(ug, su, ru)
    u_ref[...] = ug[...].reshape(modes, LANES)
    scatter_sent(part.at[0], got1, s1, r1)
    gather_sent(mg, sm, rm)
    gather_sent(ug, su, ru)
    scatter_sent(part.at[1], got2, s2, r2)
    gather_wait(ag, sa, ra)
    a_ref[...] = ag[...].reshape(modes, LANES)
    gather_wait(hg, sh, rh)
    h_ref[...] = hg[...].reshape(modes, LANES)
    gather_sent(ag, sa, ra)
    gather_sent(hg, sh, rh)
    for j in range(steps):
        out_copy(j).wait()


def gradient_kernel(dims, cells_all, a_ref, u_ref, h_ref, ph_ref, loc_ref, l_ref, sy_ref,
                    o_ref, gs_ref, lhs, turn, rhs, phase, ut, ht):
    chans, mx, my, mz, ylines, zlines, nx, ty, count, cols, owners = dims
    modes = my * mz
    steps = ylines // ty
    j = pl.program_id(0)
    me = lax.axis_index("row") * cols + lax.axis_index("col")

    @pl.when(j == 0)
    def _():
        place = lax.broadcasted_iota(jnp.int32, (modes, count), 1) == me
        found = []
        for k in range(2):
            column = jnp.sum(jnp.where(place, ph_ref[:, k * count : (k + 1) * count], 0.0), axis=1, keepdims=True)
            found.append(jnp.broadcast_to(column, (modes, LANES)))
            phase[k] = jnp.broadcast_to(ph_ref[:, 4 * count + k : 4 * count + k + 1], (modes, LANES))
        m = a_ref[...]
        im = times_i(m)
        turn[0] = m * found[0] + im * found[1]
        turn[1] = im * found[0] - m * found[1]
        ut[...] = u_ref[...].T
        ht[...] = h_ref[...].T

    mode_rhs(turn, rhs)
    synthesise(sy_ref, rhs, lhs)
    turn_on(turn, phase.at[0], phase.at[1])
    blocks = 2 * chans * chans // steps
    wave = lax.broadcasted_iota(jnp.int32, (mx, modes), 0)
    factor = jnp.where(wave == 0, 1.0 / cells_all, 2.0 / cells_all).astype(f32)

    def weight(b):
        at = j * blocks + b
        k, i, o = at // (chans * chans), at // chans % chans, at % chans

        def rows_of(ref, kind, c):
            row = (c // 2 * 4 + kind * 2 + c % 2) * mx
            return ref[pl.ds(pl.multiple_of(row, mx), mx), :]

        ur, ui, hr, hi = rows_of(ut, 0, i), rows_of(ut, 1, i), rows_of(ht, 0, o), rows_of(ht, 1, o)
        value = jnp.where(k == 0, ur * hr + ui * hi, ur * hi - ui * hr) * factor
        for q in range(my):
            lo = q * mz // LANES * LANES
            shift = q * mz - lo
            half = value[:, lo : lo + LANES]
            moved = pltpu.roll(half, LANES - shift, 1) if shift else half
            gs_ref[b * mx : (b + 1) * mx, q, :] = moved[:, :mz]

    share = -(-blocks // chans)
    for i in range(chans):
        out = back_to_x(lhs, l_ref, i)
        o_ref[0, i] = loc_ref[0, i] + out.reshape(ty, zlines, nx)
        for b in range(i * share, min((i + 1) * share, blocks)):
            weight(b)


def solution(mesh):
    nrow, ncol = mesh.shape["row"], mesh.shape["col"]
    count = nrow * ncol

    def per_device(fields, cotangent, spec_weights, point_weights, bias):
        _, chans, ylines, zlines, nx = fields.shape
        _, _, _, mx, my, mz = spec_weights.shape
        ny, nz = ylines * nrow, zlines * ncol
        modes = my * mz
        owners = min(count, modes // ROWS)
        cells_all = float(nx * ny * nz)
        ty = max(1, min(ylines, TILE // zlines))
        steps = ylines // ty
        tile = ty * zlines
        dims = (chans, mx, my, mz, ylines, zlines, nx, ty, count, ncol, owners)
        wt_tab, l_tab = x_tables(chans, nx, mx, cells_all)
        an_tab, sy_tab, ph_tab = yz_tables(ny, nz, my, mz, ty, ylines, zlines, nrow, ncol)
        flat = (2 * chans * chans * mx, my, mz)
        weights = spec_weights.reshape(flat)

        anyspace = pl.BlockSpec(memory_space=pl.ANY)
        vmem = pl.BlockSpec(memory_space=pltpu.VMEM)
        smem = pl.BlockSpec(memory_space=pltpu.SMEM)
        field_shape = jax.ShapeDtypeStruct(fields.shape, f32)
        mode_shape = jax.ShapeDtypeStruct((modes, LANES), f32)
        block = fields.shape[1:]
        gathered = pltpu.VMEM((owners, ROWS, LANES), f32)
        arrived = pltpu.VMEM((count, ROWS, LANES), f32)
        tables = [
            pltpu.VMEM((2 * chans * nx, 2 * LANES), bf16),
            pltpu.VMEM((2 * LANES, 2 * nx), bf16),
            pltpu.VMEM((2 * modes, 2 * tile), bf16),
            pltpu.VMEM((tile, 4 * modes), bf16),
        ]
        lhs_v = pltpu.VMEM((2, tile, 2 * LANES), bf16)
        turn_v = pltpu.VMEM((2, modes, LANES), f32)
        rhs_v = pltpu.VMEM((2 * modes, 2 * LANES), bf16)
        dma = pltpu.SemaphoreType.DMA

        local, adjoint, spectrum_u, spectrum_h = pl.pallas_call(
            functools.partial(layer_kernel, dims),
            out_shape=(field_shape, mode_shape, mode_shape, mode_shape),
            in_specs=[anyspace, anyspace, anyspace, smem, smem, anyspace, anyspace, anyspace, anyspace, vmem],
            out_specs=(anyspace, vmem, vmem, vmem),
            scratch_shapes=[
                pltpu.VMEM(block, f32), pltpu.VMEM(block, f32), pltpu.VMEM(block, f32),
                pltpu.VMEM((flat[0], 8, mz), f32),
                pltpu.VMEM((flat[0] // LANES, mz, LANES), f32),
                *tables,
                pltpu.VMEM((tile, 2 * chans * nx), bf16), lhs_v,
                pltpu.VMEM((2, modes, LANES), f32), turn_v, rhs_v,
                pltpu.VMEM((6, modes, LANES), f32),
                pltpu.VMEM((2, owners, ROWS, LANES), f32),
                arrived, arrived, gathered, gathered, gathered, gathered,
                dma((steps,)), dma((steps,)), dma((steps,)), dma((5,)),
                *[dma((count,))] * 12,
            ],
            compiler_params=pltpu.CompilerParams(
                collective_id=0, has_side_effects=True, vmem_limit_bytes=60 * 1024 * 1024),
            name="layer",
        )(fields, cotangent, weights, point_weights, bias, wt_tab, l_tab, an_tab, sy_tab, ph_tab)

        def keep(shape):
            return pl.BlockSpec(shape, lambda j: (0,) * len(shape))

        cells = pl.BlockSpec((1, chans, ty, zlines, nx), lambda j: (0, 0, j, 0, 0))
        mode = keep((modes, LANES))
        grad_fields, grad_spectral = pl.pallas_call(
            functools.partial(gradient_kernel, dims, cells_all),
            grid=(steps,),
            out_shape=(field_shape, jax.ShapeDtypeStruct(flat, f32)),
            in_specs=[mode, mode, mode, keep(ph_tab.shape), cells, keep(l_tab.shape), keep(sy_tab.shape)],
            out_specs=(cells, pl.BlockSpec((flat[0] // steps, my, mz), lambda j: (j, 0, 0))),
            scratch_shapes=[
                lhs_v, turn_v, rhs_v, pltpu.VMEM((2, modes, LANES), f32),
                pltpu.VMEM((LANES, modes), f32), pltpu.VMEM((LANES, modes), f32),
            ],
            compiler_params=pltpu.CompilerParams(
                dimension_semantics=("arbitrary",), vmem_limit_bytes=56 * 1024 * 1024),
            name="gradients",
        )(adjoint, spectrum_u, spectrum_h, ph_tab, local, l_tab, sy_tab)
        return grad_fields, grad_spectral.reshape(spec_weights.shape)

    placed = (P(None, None, "row", "col", None), P(None, None, "row", "col", None), P(), P(), P())
    return jax.shard_map(
        per_device,
        mesh=mesh,
        in_specs=placed,
        out_specs=(P(None, None, "row", "col", None), P()),
        check_vma=False,
    )
```

```python
import functools
import math

import jax
import jax.numpy as jnp
import numpy as np
from jax import lax
from jax.experimental import pallas as pl
from jax.experimental.pallas import tpu as pltpu
from jax.sharding import PartitionSpec as P

f32 = jnp.float32
bf16 = jnp.bfloat16
MESH = pl.DeviceIdType.MESH
TILE = 512
ROWS = 8
LANES = 128


def split(value):
    high = value.astype(bf16)
    return high, (value - high.astype(f32)).astype(bf16)


def split_np(value):
    value = np.asarray(value, np.float32)
    high = value.astype(jnp.bfloat16)
    low = (value - high.astype(np.float32)).astype(jnp.bfloat16)
    return high, low


def signed(number):
    wave = np.arange(number)
    return np.where(wave < number // 2, wave, wave - number)


def x_tables(chans, length, modes, cells):
    angle = 2.0 * np.pi / length * ((np.arange(length)[:, None] * np.arange(modes)) % length)
    weight = np.where(np.arange(modes) == 0, 1.0, 2.0) / cells
    first = np.stack([np.cos(angle), -np.sin(angle)], 1)
    eye = np.eye(chans).reshape(chans, chans // 2, 2)
    wide = np.einsum("cgd,xkp->cxgkdp", eye, first).reshape(chans, 1, length, -1)
    wide = np.repeat(wide, 2, 1).reshape(2 * chans * length, -1)
    tall = np.einsum("de,xkp->kdpex", np.eye(2), first * weight).reshape(-1, 2 * length)
    high, low = split_np(tall)
    return np.concatenate(split_np(wide), 1), np.concatenate([high, high, low, 0 * low], 0)


def yz_tables(ny, nz, my, mz, ty, ylines, zlines, nrow, ncol):
    ky, kz = np.repeat(signed(my), mz), np.tile(signed(mz), my)

    def turns(y, z):
        return ((np.outer(y, ky) % ny) / ny + (np.outer(z, kz) % nz) / nz) * 2.0 * np.pi

    angle = turns(np.repeat(np.arange(ty), zlines), np.tile(np.arange(zlines), ty))
    high, low = split_np(np.concatenate([np.cos(angle), np.sin(angle)], 1))
    device_y = np.repeat(np.arange(nrow) * ylines, ncol)
    device_z = np.tile(np.arange(ncol) * zlines, nrow)
    start = turns(device_y, device_z).T
    end = turns(device_y + ylines - ty, device_z).T
    step = turns(np.array([ty]), np.array([0])).T
    phase = np.concatenate(
        [np.cos(start), np.sin(start), np.cos(end), np.sin(end), np.cos(step), np.sin(step)], 1)
    return (np.concatenate([high.T, low.T], 1), np.concatenate([high, low], 1),
            phase.astype(np.float32))


def dot(a, b):
    return jnp.dot(a, b, preferred_element_type=f32)


def lane_ids(rows):
    return lax.broadcasted_iota(jnp.int32, (rows, LANES), 1)


def times_i(value):
    quarter = LANES // 4
    real = lane_ids(value.shape[0]) % (LANES // 2) < quarter
    return jnp.where(real, -pltpu.roll(value, LANES - quarter, 1), pltpu.roll(value, quarter, 1))


def along_x(value, c, xs, wt_v):
    width = value.shape[1]
    at = 2 * c * width
    high, low = split(value)
    xs[:, at : at + width] = high
    xs[:, at + width : at + 2 * width] = low
    return dot(xs[:, at : at + 2 * width], wt_v[at : at + 2 * width, :])


def analyse(pairs, an_v, acc, step_cos, step_sin):
    part = jnp.concatenate(split(pairs[:, :LANES] + pairs[:, LANES:]), 1)
    both = dot(an_v[...], jnp.concatenate([part, part], 0))
    both = both[:, :LANES] + both[:, LANES:]
    modes = both.shape[0] // 2
    c, s = acc[0], acc[1]
    new_c = c * step_cos[...] + s * step_sin[...] + both[:modes]
    new_s = s * step_cos[...] - c * step_sin[...] + both[modes:]
    acc[0] = new_c
    acc[1] = new_s


def spectrum(acc, end_cos, end_sin):
    c, s = acc[0], acc[1]
    cosine = c * end_cos[...] - s * end_sin[...]
    sine = s * end_cos[...] + c * end_sin[...]
    return cosine - times_i(sine)


def mode_rhs(turn, rhs):
    modes = turn.shape[1]
    for k in range(2):
        high, low = split(turn[k])
        rhs[k * modes : (k + 1) * modes, :LANES] = high
        rhs[k * modes : (k + 1) * modes, LANES:] = low


def turn_on(turn, step_cos, step_sin):
    m, im = turn[0], turn[1]
    turn[0] = m * step_cos[...] + im * step_sin[...]
    turn[1] = im * step_cos[...] - m * step_sin[...]


def synthesise(sy_v, rhs, lhs):
    pairs = dot(sy_v[...], jnp.concatenate([rhs[...], rhs[...]], 0))
    value = pairs[:, :LANES] + pairs[:, LANES:]
    other = pltpu.roll(value, LANES // 2, 1)
    lower = lane_ids(value.shape[0]) < LANES // 2
    for pair in range(2):
        twice = jnp.where(lower, value, other) if pair == 0 else jnp.where(lower, other, value)
        high = twice.astype(bf16)
        wide = high.astype(f32)
        lhs[pair, :, :LANES] = jnp.where(lower, wide, twice - wide).astype(bf16)
        lhs[pair, :, LANES:] = high


def back_to_x(lhs, l_v, c):
    nx = l_v.shape[1] // 2
    return dot(lhs[c // 2], l_v[:, c % 2 * nx : (c % 2 + 1) * nx])


def gelu_slope(v):
    arg = v * math.sqrt(0.5)
    gauss = jnp.exp2(arg * arg * (-1.0 / math.log(2.0)))
    return (0.5 * lax.erf(arg) + 0.5) + (v * (1.0 / math.sqrt(2.0 * math.pi))) * gauss


def layer_kernel(dims, f_hbm, g_hbm, w_hbm, pw, bias, wt_hbm, l_hbm, an_hbm, sy_hbm, ph_ref,
                 loc_o, u_ref, h_ref, wd_ref,
                 f_v, g_v, w_v, wt_v, l_v, an_v, sy_v, xs, lhs, acc, turn, rhs,
                 phase, part, got1, got2, mg, ug, hg,
                 f_sem, g_sem, tab_sem,
                 s1, r1, sm, rm, su, ru, s2, r2, sh, rh):
    chans, mx, my, mz, ylines, zlines, nx, ty, count, cols, owners = dims
    modes = my * mz
    steps = ylines // ty
    tile = ty * zlines
    loc_v = loc_o.at[0]
    me = lax.axis_index("row") * cols + lax.axis_index("col")

    def device(t):
        return {"row": t // cols, "col": lax.rem(t, cols)}

    barrier = pltpu.get_barrier_semaphore()

    def greet(k, carry):
        pl.semaphore_signal(barrier, inc=1, device_id=device(lax.rem(me + k, count)), device_id_type=MESH)
        return carry

    lax.fori_loop(1, count, greet, 0)

    q = jnp.minimum(me, owners - 1) * ROWS // mz
    r0 = pl.multiple_of(lax.rem(jnp.minimum(me, owners - 1) * ROWS, mz), ROWS)

    def tile_copy(src, dst, sem, j):
        rows = pl.ds(j * ty, ty)
        return pltpu.make_async_copy(src.at[0, :, rows], dst.at[:, rows], sem.at[j])

    wt_copy = pltpu.make_async_copy(wt_hbm, wt_v, tab_sem.at[0])
    l_copy = pltpu.make_async_copy(l_hbm, l_v, tab_sem.at[1])
    an_copy = pltpu.make_async_copy(an_hbm, an_v, tab_sem.at[2])
    sy_copy = pltpu.make_async_copy(sy_hbm, sy_v, tab_sem.at[3])
    w_copy = pltpu.make_async_copy(w_hbm, w_v, tab_sem.at[4])
    wt_copy.start()
    tile_copy(f_hbm, f_v, f_sem, 0).start()
    an_copy.start()
    for j in range(1, steps):
        tile_copy(f_hbm, f_v, f_sem, j).start()
    w_copy.start()
    sy_copy.start()
    l_copy.start()
    for j in range(steps):
        tile_copy(g_hbm, g_v, g_sem, j).start()

    place = lax.broadcasted_iota(jnp.int32, (modes, count), 1) == me
    for k in range(4):
        column = jnp.sum(jnp.where(place, ph_ref[:, k * count : (k + 1) * count], 0.0), axis=1, keepdims=True)
        phase[k] = jnp.broadcast_to(column, (modes, LANES))
    for k in range(2):
        phase[4 + k] = jnp.broadcast_to(ph_ref[:, 4 * count + k : 4 * count + k + 1], (modes, LANES))
    start_cos, start_sin, end_cos, end_sin, step_cos, step_sin = [phase.at[k] for k in range(6)]
    acc[...] = jnp.zeros_like(acc)

    wt_copy.wait()
    an_copy.wait()

    def first(j, carry):
        tile_copy(f_hbm, f_v, f_sem, j).wait()

        pairs = 0.0
        for c in range(chans):
            pairs += along_x(f_v[c, pl.ds(j * ty, ty)].reshape(tile, nx), c, xs, wt_v)
        analyse(pairs, an_v, acc, step_cos, step_sin)
        return carry

    lax.fori_loop(0, steps, first, 0)
    part[0] = spectrum(acc, end_cos, end_sin).reshape(owners, ROWS, LANES)
    pl.semaphore_wait(barrier, count - 1)

    def piece(src, dst, send, recv, k, arriving, scatter):
        t = lax.rem(me + k, count)
        slot = t if arriving else me
        return pltpu.make_async_remote_copy(
            src_ref=src.at[t if scatter else me], dst_ref=dst.at[slot], send_sem=send.at[t],
            recv_sem=recv.at[slot], device_id=device(t), device_id_type=MESH)

    def each(action):
        def body(k, carry):
            action(k)
            return carry
        lax.fori_loop(1, count, body, 0)

    def owned(k, action):
        if owners == count:
            action()
        else:
            pl.when(lax.rem(me + k, count) < owners)(action)

    def owner(action):
        if owners == count:
            action()
        else:
            pl.when(me < owners)(action)

    def scatter_start(src, dst, send, recv):
        each(lambda k: owned(k, lambda: piece(src, dst, send, recv, k, False, True).start()))

    def scatter_sent(src, dst, send, recv):
        each(lambda k: owned(k, lambda: piece(src, dst, send, recv, k, False, True).wait_send()))

    def scatter_sum(src, dst, send, recv):
        each(lambda k: piece(src, dst, send, recv, k, True, False).wait_recv())
        dst[pl.ds(me, 1)] = src[pl.ds(me, 1)]
        return jnp.sum(dst[...], axis=0)

    def gather_start(ref, send, recv):
        each(lambda k: piece(ref, ref, send, recv, k, False, False).start())

    def gather_wait(ref, send, recv):
        each(lambda k: owned(k, lambda: piece(ref, ref, send, recv, k, True, False).wait_recv()))

    def gather_sent(ref, send, recv):
        owner(lambda: each(lambda k: piece(ref, ref, send, recv, k, False, False).wait_send()))

    scatter_start(part.at[0], got1, s1, r1)

    w_copy.wait()
    rows_w = chans * mx * 2
    for b in range(w_v.shape[0] // rows_w):
        wd_ref[b, pl.ds(pl.multiple_of(q * mz, mz), mz), :] = w_v[rows_w * b : rows_w * (b + 1), q, :].T

    step = 16
    per = zlines // step

    def local(k, carry):
        y, z = k // per, k % per
        zs = pl.ds(pl.multiple_of(z * step, step), step)
        fields = [f_v[i, y, zs, :] for i in range(chans)]
        for o in range(chans):
            total = fields[0] * pw[0, o] + bias[o]
            for i in range(1, chans):
                total += fields[i] * pw[i, o]
            loc_v[o, y, zs, :] = total
        return carry

    lax.fori_loop(0, ylines * per, local, 0)

    lane = lane_ids(ROWS)
    quarter = LANES // 4
    is_real = lane % (LANES // 2) < quarter
    wave = lane % mx

    def lane_of(kind, chan):
        return chan // 2 * (LANES // 2) + kind * quarter + chan % 2 * mx + wave

    def take(value, index):
        return jnp.take_along_axis(value, index, axis=1)

    def weights():
        return [wd_ref[b, pl.ds(pl.multiple_of(q * mz + r0, ROWS), ROWS), :] for b in range(chans)]

    def mix_first():
        u = scatter_sum(part.at[0], got1, s1, r1)
        ug[pl.ds(me, 1)] = u[None]
        w = weights()
        real = imag = 0.0
        for pair in range(2):
            chan = 2 * pair + lane // (LANES // 2)
            ur, ui = take(u, lane_of(0, chan)), take(u, lane_of(1, chan))
            wr, wi = w[pair], w[2 + pair]
            real += wr * ur - wi * ui
            imag += wr * ui + wi * ur
        real += pltpu.roll(real, LANES // 2, 1)
        imag += pltpu.roll(imag, LANES // 2, 1)
        source = lane // (LANES // 2) * quarter + lane % quarter
        mg[pl.ds(me, 1)] = jnp.where(is_real, take(real, source), take(imag, source))[None]
        gather_start(mg, sm, rm)
        gather_start(ug, su, ru)

    owner(mix_first)

    def relay(k, carry):
        row = pl.multiple_of(k * mz, mz)
        for b in range(chans):
            wd_ref[b, pl.ds(row, mz), :] = w_v[rows_w * b : rows_w * (b + 1), k, :].T
        return carry

    lax.fori_loop(0, my, relay, 0)
    sy_copy.wait()
    l_copy.wait()
    gather_wait(mg, sm, rm)

    def load_turn(ref):
        m = ref[...].reshape(modes, LANES)
        im = times_i(m)
        turn[0] = m * start_cos[...] + im * start_sin[...]
        turn[1] = im * start_cos[...] - m * start_sin[...]

    load_turn(mg)
    acc[...] = jnp.zeros_like(acc)

    def second(j, carry):
        mode_rhs(turn, rhs)
        synthesise(sy_v, rhs, lhs)
        turn_on(turn, step_cos, step_sin)
        tile_copy(g_hbm, g_v, g_sem, j).wait()
        lines = pl.ds(j * ty, ty)
        pairs = 0.0
        for o in range(chans):
            pre = back_to_x(lhs, l_v, o) + loc_v[o, lines].reshape(tile, nx)
            up = g_v[o, lines].reshape(tile, nx) * gelu_slope(pre)
            g_v[o, lines] = up.reshape(ty, zlines, nx)
            pairs += along_x(up, o, xs, wt_v)
        analyse(pairs, an_v, acc, step_cos, step_sin)
        return carry

    lax.fori_loop(0, steps, second, 0)
    part[1] = spectrum(acc, end_cos, end_sin).reshape(owners, ROWS, LANES)
    scatter_start(part.at[1], got2, s2, r2)

    def back(j, carry):
        def cells(k, carry):
            y, z = j * ty + k // per, k % per
            zs = pl.ds(pl.multiple_of(z * step, step), step)
            ups = [g_v[o, y, zs, :] for o in range(chans)]
            for i in range(chans):
                total = ups[0] * pw[i, 0]
                for o in range(1, chans):
                    total += ups[o] * pw[i, o]
                loc_v[i, y, zs, :] = total
            return carry

        lax.fori_loop(0, ty * per, cells, 0)
        return carry

    lax.fori_loop(0, steps, back, 0)

    def last():
        hg[pl.ds(me, 1)] = scatter_sum(part.at[1], got2, s2, r2)[None]
        gather_start(hg, sh, rh)

    owner(last)
    gather_wait(ug, su, ru)
    u_ref[...] = ug[...].reshape(modes, LANES)
    scatter_sent(part.at[0], got1, s1, r1)
    gather_sent(mg, sm, rm)
    gather_sent(ug, su, ru)
    scatter_sent(part.at[1], got2, s2, r2)
    gather_wait(hg, sh, rh)
    h_ref[...] = hg[...].reshape(modes, LANES)
    gather_sent(hg, sh, rh)


def lane_of(kind, chan, wave, width):
    return chan // 2 * (LANES // 2) + kind * (LANES // 4) + chan % 2 * width + wave


def adjoint(h, weights, chans, mx):
    lane = lane_ids(h.shape[0])
    wave, quarter = lane % mx, LANES // 4
    is_real = lane % (LANES // 2) < quarter

    def take(value, index):
        return jnp.take_along_axis(value, index, axis=1)

    chan = lane // mx % chans
    hr, hi = take(h, lane_of(0, chan, wave, mx)), take(h, lane_of(1, chan, wave, mx))
    index = lane % quarter // mx * (LANES // 2) + (chans - 1) * mx + wave
    result = jnp.zeros_like(h)
    for pair in range(2):
        wr, wi = weights[pair], weights[2 + pair]
        for k, value in enumerate((wr * hr + wi * hi, wr * hi - wi * hr)):
            total = value
            for o in range(1, chans):
                total += pltpu.roll(value, o * mx, 1)
            here = (is_real if k == 0 else jnp.logical_not(is_real)) & (lane // (LANES // 2) == pair)
            result = jnp.where(here, take(total, index), result)
    return result


def gradient_kernel(dims, cells_all, u_ref, h_ref, wd_ref, ph_ref, loc_ref, l_ref, sy_ref,
                    o_ref, gs_ref, lhs, turn, rhs, phase, ut, ht):
    chans, mx, my, mz, ylines, zlines, nx, ty, count, cols, owners = dims
    modes = my * mz
    steps = ylines // ty
    j = pl.program_id(0)
    me = lax.axis_index("row") * cols + lax.axis_index("col")

    @pl.when(j == 0)
    def _():
        place = lax.broadcasted_iota(jnp.int32, (modes, count), 1) == me
        found = []
        for k in range(2):
            column = jnp.sum(jnp.where(place, ph_ref[:, k * count : (k + 1) * count], 0.0), axis=1, keepdims=True)
            found.append(jnp.broadcast_to(column, (modes, LANES)))
            phase[k] = jnp.broadcast_to(ph_ref[:, 4 * count + k : 4 * count + k + 1], (modes, LANES))
        m = adjoint(h_ref[...], [wd_ref[b] for b in range(chans)], chans, mx)
        im = times_i(m)
        turn[0] = m * found[0] + im * found[1]
        turn[1] = im * found[0] - m * found[1]
        ut[...] = u_ref[...].T
        ht[...] = h_ref[...].T

    mode_rhs(turn, rhs)
    synthesise(sy_ref, rhs, lhs)
    turn_on(turn, phase.at[0], phase.at[1])
    blocks = 2 * chans * chans // steps
    wave = lax.broadcasted_iota(jnp.int32, (mx, modes), 0)
    factor = jnp.where(wave == 0, 1.0 / cells_all, 2.0 / cells_all).astype(f32)

    def weight(b):
        at = j * blocks + b
        k, i, o = at // (chans * chans), at // chans % chans, at % chans

        def rows_of(ref, kind, c):
            row = (c // 2 * 4 + kind * 2 + c % 2) * mx
            return ref[pl.ds(pl.multiple_of(row, mx), mx), :]

        ur, ui, hr, hi = rows_of(ut, 0, i), rows_of(ut, 1, i), rows_of(ht, 0, o), rows_of(ht, 1, o)
        value = jnp.where(k == 0, ur * hr + ui * hi, ur * hi - ui * hr) * factor
        for q in range(my):
            lo = q * mz // LANES * LANES
            shift = q * mz - lo
            half = value[:, lo : lo + LANES]
            moved = pltpu.roll(half, LANES - shift, 1) if shift else half
            gs_ref[b * mx : (b + 1) * mx, q, :] = moved[:, :mz]

    share = -(-blocks // chans)
    for i in range(chans):
        out = back_to_x(lhs, l_ref, i)
        o_ref[0, i] = loc_ref[0, i, pl.ds(j * ty, ty)] + out.reshape(ty, zlines, nx)
        for b in range(i * share, min((i + 1) * share, blocks)):
            weight(b)


def solution(mesh):
    nrow, ncol = mesh.shape["row"], mesh.shape["col"]
    count = nrow * ncol

    def per_device(fields, cotangent, spec_weights, point_weights, bias):
        _, chans, ylines, zlines, nx = fields.shape
        _, _, _, mx, my, mz = spec_weights.shape
        ny, nz = ylines * nrow, zlines * ncol
        modes = my * mz
        owners = min(count, modes // ROWS)
        cells_all = float(nx * ny * nz)
        ty = max(1, min(ylines, TILE // zlines))
        steps = ylines // ty
        tile = ty * zlines
        dims = (chans, mx, my, mz, ylines, zlines, nx, ty, count, ncol, owners)
        wt_tab, l_tab = x_tables(chans, nx, mx, cells_all)
        an_tab, sy_tab, ph_tab = yz_tables(ny, nz, my, mz, ty, ylines, zlines, nrow, ncol)
        flat = (2 * chans * chans * mx, my, mz)
        weights = spec_weights.reshape(flat)

        anyspace = pl.BlockSpec(memory_space=pl.ANY)
        vmem = pl.BlockSpec(memory_space=pltpu.VMEM)
        smem = pl.BlockSpec(memory_space=pltpu.SMEM)
        field_shape = jax.ShapeDtypeStruct(fields.shape, f32)
        mode_shape = jax.ShapeDtypeStruct((modes, LANES), f32)
        block = fields.shape[1:]
        gathered = pltpu.VMEM((owners, ROWS, LANES), f32)
        arrived = pltpu.VMEM((count, ROWS, LANES), f32)
        tables = [
            pltpu.VMEM((2 * chans * nx, 2 * LANES), bf16),
            pltpu.VMEM((2 * LANES, 2 * nx), bf16),
            pltpu.VMEM((2 * modes, 2 * tile), bf16),
            pltpu.VMEM((tile, 4 * modes), bf16),
        ]
        lhs_v = pltpu.VMEM((2, tile, 2 * LANES), bf16)
        turn_v = pltpu.VMEM((2, modes, LANES), f32)
        rhs_v = pltpu.VMEM((2 * modes, 2 * LANES), bf16)
        dma = pltpu.SemaphoreType.DMA

        local, spectrum_u, spectrum_h, wide_w = pl.pallas_call(
            functools.partial(layer_kernel, dims),
            out_shape=(pltpu.VMEM(fields.shape, f32),) + (pltpu.VMEM((modes, LANES), f32),) * 2
            + (pltpu.VMEM((4, modes, LANES), f32),),
            in_specs=[anyspace, anyspace, anyspace, smem, smem, anyspace, anyspace, anyspace, anyspace, vmem],
            out_specs=(vmem, vmem, vmem, vmem),
            scratch_shapes=[
                pltpu.VMEM(block, f32), pltpu.VMEM(block, f32),
                pltpu.VMEM(flat, f32),
                *tables,
                pltpu.VMEM((tile, 2 * chans * nx), bf16), lhs_v,
                pltpu.VMEM((2, modes, LANES), f32), turn_v, rhs_v,
                pltpu.VMEM((6, modes, LANES), f32),
                pltpu.VMEM((2, owners, ROWS, LANES), f32),
                arrived, arrived, gathered, gathered, gathered,
                dma((steps,)), dma((steps,)), dma((5,)),
                *[dma((count,))] * 10,
            ],
            compiler_params=pltpu.CompilerParams(
                collective_id=0, has_side_effects=True, vmem_limit_bytes=46 * 1024 * 1024),
            name="layer",
        )(*[pltpu.with_memory_space_constraint(x, pltpu.HBM) for x in (fields, cotangent, weights)],
          point_weights, bias,
          *[pltpu.with_memory_space_constraint(jnp.asarray(x), pltpu.HBM) for x in (wt_tab, l_tab, an_tab, sy_tab)], ph_tab)

        def keep(shape):
            return pl.BlockSpec(shape, lambda j: (0,) * len(shape))

        cells = pl.BlockSpec((1, chans, ty, zlines, nx), lambda j: (0, 0, j, 0, 0))
        mode = keep((modes, LANES))
        grad_fields, grad_spectral = pl.pallas_call(
            functools.partial(gradient_kernel, dims, cells_all),
            grid=(steps,),
            out_shape=(field_shape, jax.ShapeDtypeStruct(flat, f32)),
            in_specs=[mode, mode, keep((4, modes, LANES)), keep(ph_tab.shape), vmem, keep(l_tab.shape), keep(sy_tab.shape)],
            out_specs=(cells, pl.BlockSpec((flat[0] // steps, my, mz), lambda j: (j, 0, 0))),
            scratch_shapes=[
                lhs_v, turn_v, rhs_v, pltpu.VMEM((2, modes, LANES), f32),
                pltpu.VMEM((LANES, modes), f32), pltpu.VMEM((LANES, modes), f32),
            ],
            compiler_params=pltpu.CompilerParams(
                dimension_semantics=("arbitrary",), vmem_limit_bytes=36 * 1024 * 1024),
            name="gradients",
        )(spectrum_u, spectrum_h, wide_w, ph_tab, local, l_tab, sy_tab)
        return grad_fields, grad_spectral.reshape(spec_weights.shape)

    placed = (P(None, None, "row", "col", None), P(None, None, "row", "col", None), P(), P(), P())
    return jax.shard_map(
        per_device,
        mesh=mesh,
        in_specs=placed,
        out_specs=(P(None, None, "row", "col", None), P()),
        check_vma=False,
    )
```

```python
import functools
import math

import jax
import jax.numpy as jnp
import numpy as np
from jax import lax
from jax.experimental import pallas as pl
from jax.experimental.pallas import tpu as pltpu
from jax.sharding import PartitionSpec as P

f32 = jnp.float32
bf16 = jnp.bfloat16
MESH = pl.DeviceIdType.MESH
TILE = 512
ROWS = 8
LANES = 128
HALF_ROOT = math.sqrt(0.5)


def split(value):
    high = value.astype(bf16)
    return high, (value - high.astype(f32)).astype(bf16)


def split_np(value):
    value = np.asarray(value, np.float32)
    high = value.astype(jnp.bfloat16)
    low = (value - high.astype(np.float32)).astype(jnp.bfloat16)
    return high, low


def signed(number):
    wave = np.arange(number)
    return np.where(wave < number // 2, wave, wave - number)


def x_tables(chans, length, modes, cells):
    angle = 2.0 * np.pi / length * ((np.arange(length)[:, None] * np.arange(modes)) % length)
    weight = np.where(np.arange(modes) == 0, 1.0, 2.0) / cells * HALF_ROOT
    first = np.stack([np.cos(angle), -np.sin(angle)], 1)
    eye = np.eye(chans).reshape(chans, chans // 2, 2)
    wide = np.einsum("cgd,xkp->cxgkdp", eye, first).reshape(chans, 1, length, -1)
    wide = np.repeat(wide, 2, 1).reshape(2 * chans * length, -1)
    tall = np.einsum("de,xkp->kdpex", np.eye(2), first * weight).reshape(-1, 2 * length)
    high, low = split_np(tall)
    return np.concatenate(split_np(wide), 1), np.concatenate([high, high, low, 0 * low], 0)


def yz_tables(ny, nz, my, mz, ty, ylines, zlines, nrow, ncol):
    ky, kz = np.repeat(signed(my), mz), np.tile(signed(mz), my)

    def turns(y, z):
        return ((np.outer(y, ky) % ny) / ny + (np.outer(z, kz) % nz) / nz) * 2.0 * np.pi

    angle = turns(np.repeat(np.arange(ty), zlines), np.tile(np.arange(zlines), ty))
    high, low = split_np(np.concatenate([np.cos(angle), np.sin(angle)], 1))
    device_y = np.repeat(np.arange(nrow) * ylines, ncol)
    device_z = np.tile(np.arange(ncol) * zlines, nrow)
    start = turns(device_y, device_z).T
    end = turns(device_y + ylines - ty, device_z).T
    step = turns(np.array([ty]), np.array([0])).T
    phase = np.concatenate(
        [np.cos(start), np.sin(start), np.cos(end), np.sin(end), np.cos(step), np.sin(step)], 1)
    return (np.concatenate([high.T, low.T], 1), np.concatenate([high, low], 1),
            phase.astype(np.float32))


def dot(a, b):
    return jnp.dot(a, b, preferred_element_type=f32)


def lane_ids(rows):
    return lax.broadcasted_iota(jnp.int32, (rows, LANES), 1)


def times_i(value):
    quarter = LANES // 4
    real = lane_ids(value.shape[0]) % (LANES // 2) < quarter
    return jnp.where(real, -pltpu.roll(value, LANES - quarter, 1), pltpu.roll(value, quarter, 1))


def along_x(value, c, xs, wt_v):
    width = value.shape[1]
    at = 2 * c * width
    high, low = split(value)
    xs[:, at : at + width] = high
    xs[:, at + width : at + 2 * width] = low
    return dot(xs[:, at : at + 2 * width], wt_v[at : at + 2 * width, :])


def analyse(pairs, an_v, acc, step_cos, step_sin):
    part = jnp.concatenate(split(pairs[:, :LANES] + pairs[:, LANES:]), 1)
    both = dot(an_v[...], jnp.concatenate([part, part], 0))
    both = both[:, :LANES] + both[:, LANES:]
    modes = both.shape[0] // 2
    c, s = acc[0], acc[1]
    new_c = c * step_cos[...] + s * step_sin[...] + both[:modes]
    new_s = s * step_cos[...] - c * step_sin[...] + both[modes:]
    acc[0] = new_c
    acc[1] = new_s


def spectrum(acc, end_cos, end_sin):
    c, s = acc[0], acc[1]
    cosine = c * end_cos[...] - s * end_sin[...]
    sine = s * end_cos[...] + c * end_sin[...]
    return cosine - times_i(sine)


def mode_rhs(turn, rhs):
    modes = turn.shape[1]
    for k in range(2):
        high, low = split(turn[k])
        rhs[k * modes : (k + 1) * modes, :LANES] = high
        rhs[k * modes : (k + 1) * modes, LANES:] = low


def turn_on(turn, step_cos, step_sin):
    m, im = turn[0], turn[1]
    turn[0] = m * step_cos[...] + im * step_sin[...]
    turn[1] = im * step_cos[...] - m * step_sin[...]


def synthesise(sy_v, rhs, lhs):
    pairs = dot(sy_v[...], jnp.concatenate([rhs[...], rhs[...]], 0))
    value = pairs[:, :LANES] + pairs[:, LANES:]
    other = pltpu.roll(value, LANES // 2, 1)
    lower = lane_ids(value.shape[0]) < LANES // 2
    for pair in range(2):
        twice = jnp.where(lower, value, other) if pair == 0 else jnp.where(lower, other, value)
        high = twice.astype(bf16)
        wide = high.astype(f32)
        lhs[pair, :, :LANES] = jnp.where(lower, wide, twice - wide).astype(bf16)
        lhs[pair, :, LANES:] = high


def back_to_x(lhs, l_v, c):
    nx = l_v.shape[1] // 2
    return dot(lhs[c // 2], l_v[:, c % 2 * nx : (c % 2 + 1) * nx])


def twice_gelu_slope(t):
    gauss = jnp.exp2(t * t * (-1.0 / math.log(2.0)))
    return (lax.erf(t) + 1.0) + (t * (2.0 / math.sqrt(math.pi))) * gauss


def layer_kernel(dims, f_hbm, g_hbm, w_hbm, pw, bias, wt_hbm, l_hbm, an_hbm, sy_hbm, ph_ref,
                 loc_o, u_ref, h_ref, wd_ref,
                 f_v, g_v, w_v, wt_v, l_v, an_v, sy_v, xs, lhs, acc, turn, rhs,
                 phase, part, got1, got2, mg, ug, hg,
                 f_sem, g_sem, tab_sem,
                 s1, r1, sm, rm, su, ru, s2, r2, sh, rh):
    chans, mx, my, mz, ylines, zlines, nx, ty, count, cols, owners = dims
    modes = my * mz
    steps = ylines // ty
    tile = ty * zlines
    loc_v = loc_o.at[0]
    me = lax.axis_index("row") * cols + lax.axis_index("col")

    def device(t):
        return {"row": t // cols, "col": lax.rem(t, cols)}

    barrier = pltpu.get_barrier_semaphore()

    def greet(k, carry):
        pl.semaphore_signal(barrier, inc=1, device_id=device(lax.rem(me + k, count)), device_id_type=MESH)
        return carry

    lax.fori_loop(1, count, greet, 0)

    q = jnp.minimum(me, owners - 1) * ROWS // mz
    r0 = pl.multiple_of(lax.rem(jnp.minimum(me, owners - 1) * ROWS, mz), ROWS)

    def tile_copy(src, dst, sem, j):
        rows = pl.ds(j * ty, ty)
        return pltpu.make_async_copy(src.at[0, :, rows], dst.at[:, rows], sem.at[j])

    wt_copy = pltpu.make_async_copy(wt_hbm, wt_v, tab_sem.at[0])
    l_copy = pltpu.make_async_copy(l_hbm, l_v, tab_sem.at[1])
    an_copy = pltpu.make_async_copy(an_hbm, an_v, tab_sem.at[2])
    sy_copy = pltpu.make_async_copy(sy_hbm, sy_v, tab_sem.at[3])
    w_copy = pltpu.make_async_copy(w_hbm, w_v, tab_sem.at[4])
    wt_copy.start()
    tile_copy(f_hbm, f_v, f_sem, 0).start()
    an_copy.start()
    for j in range(1, steps):
        tile_copy(f_hbm, f_v, f_sem, j).start()
    w_copy.start()
    sy_copy.start()
    l_copy.start()
    for j in range(steps):
        tile_copy(g_hbm, g_v, g_sem, j).start()

    place = lax.broadcasted_iota(jnp.int32, (modes, count), 1) == me
    for k in range(4):
        column = jnp.sum(jnp.where(place, ph_ref[:, k * count : (k + 1) * count], 0.0), axis=1, keepdims=True)
        phase[k] = jnp.broadcast_to(column, (modes, LANES))
    for k in range(2):
        phase[4 + k] = jnp.broadcast_to(ph_ref[:, 4 * count + k : 4 * count + k + 1], (modes, LANES))
    start_cos, start_sin, end_cos, end_sin, step_cos, step_sin = [phase.at[k] for k in range(6)]
    acc[...] = jnp.zeros_like(acc)

    wt_copy.wait()
    an_copy.wait()

    def first(j, carry):
        tile_copy(f_hbm, f_v, f_sem, j).wait()

        pairs = 0.0
        for c in range(chans):
            pairs += along_x(f_v[c, pl.ds(j * ty, ty)].reshape(tile, nx), c, xs, wt_v)
        analyse(pairs, an_v, acc, step_cos, step_sin)
        return carry

    lax.fori_loop(0, steps, first, 0)
    part[0] = spectrum(acc, end_cos, end_sin).reshape(owners, ROWS, LANES)
    pl.semaphore_wait(barrier, count - 1)

    def piece(src, dst, send, recv, k, arriving, scatter):
        t = lax.rem(me + k, count)
        slot = t if arriving else me
        return pltpu.make_async_remote_copy(
            src_ref=src.at[t if scatter else me], dst_ref=dst.at[slot], send_sem=send.at[t],
            recv_sem=recv.at[slot], device_id=device(t), device_id_type=MESH)

    def each(action):
        def body(k, carry):
            action(k)
            return carry
        lax.fori_loop(1, count, body, 0)

    def owned(k, action):
        if owners == count:
            action()
        else:
            pl.when(lax.rem(me + k, count) < owners)(action)

    def owner(action):
        if owners == count:
            action()
        else:
            pl.when(me < owners)(action)

    def scatter_start(src, dst, send, recv):
        each(lambda k: owned(k, lambda: piece(src, dst, send, recv, k, False, True).start()))

    def scatter_sent(src, dst, send, recv):
        each(lambda k: owned(k, lambda: piece(src, dst, send, recv, k, False, True).wait_send()))

    def scatter_sum(src, dst, send, recv):
        each(lambda k: piece(src, dst, send, recv, k, True, False).wait_recv())
        dst[pl.ds(me, 1)] = src[pl.ds(me, 1)]
        return jnp.sum(dst[...], axis=0)

    def gather_start(ref, send, recv):
        each(lambda k: piece(ref, ref, send, recv, k, False, False).start())

    def gather_wait(ref, send, recv):
        each(lambda k: owned(k, lambda: piece(ref, ref, send, recv, k, True, False).wait_recv()))

    def gather_sent(ref, send, recv):
        owner(lambda: each(lambda k: piece(ref, ref, send, recv, k, False, False).wait_send()))

    scatter_start(part.at[0], got1, s1, r1)

    w_copy.wait()
    rows_w = chans * mx * 2
    for b in range(w_v.shape[0] // rows_w):
        wd_ref[b, pl.ds(pl.multiple_of(q * mz, mz), mz), :] = w_v[rows_w * b : rows_w * (b + 1), q, :].T

    step = 16
    per = zlines // step

    def local(k, carry):
        y, z = k // per, k % per
        zs = pl.ds(pl.multiple_of(z * step, step), step)
        fields = [f_v[i, y, zs, :] for i in range(chans)]
        for o in range(chans):
            total = fields[0] * (pw[0, o] * HALF_ROOT) + bias[o] * HALF_ROOT
            for i in range(1, chans):
                total += fields[i] * (pw[i, o] * HALF_ROOT)
            loc_v[o, y, zs, :] = total
        return carry

    lax.fori_loop(0, ylines * per, local, 0)

    lane = lane_ids(ROWS)
    quarter = LANES // 4
    is_real = lane % (LANES // 2) < quarter
    wave = lane % mx

    def lane_of(kind, chan):
        return chan // 2 * (LANES // 2) + kind * quarter + chan % 2 * mx + wave

    def take(value, index):
        return jnp.take_along_axis(value, index, axis=1)

    def weights():
        return [wd_ref[b, pl.ds(pl.multiple_of(q * mz + r0, ROWS), ROWS), :] for b in range(chans)]

    def mix_first():
        u = scatter_sum(part.at[0], got1, s1, r1)
        ug[pl.ds(me, 1)] = u[None]
        w = weights()
        real = imag = 0.0
        for pair in range(2):
            chan = 2 * pair + lane // (LANES // 2)
            ur, ui = take(u, lane_of(0, chan)), take(u, lane_of(1, chan))
            wr, wi = w[pair], w[2 + pair]
            real += wr * ur - wi * ui
            imag += wr * ui + wi * ur
        real += pltpu.roll(real, LANES // 2, 1)
        imag += pltpu.roll(imag, LANES // 2, 1)
        source = lane // (LANES // 2) * quarter + lane % quarter
        mg[pl.ds(me, 1)] = jnp.where(is_real, take(real, source), take(imag, source))[None]
        gather_start(mg, sm, rm)

    owner(mix_first)

    def relay(k, carry):
        row = pl.multiple_of(k * mz, mz)
        for b in range(chans):
            wd_ref[b, pl.ds(row, mz), :] = w_v[rows_w * b : rows_w * (b + 1), k, :].T
        return carry

    lax.fori_loop(0, my, relay, 0)
    sy_copy.wait()
    l_copy.wait()
    gather_wait(mg, sm, rm)
    owner(lambda: gather_start(ug, su, ru))

    def load_turn(ref):
        m = ref[...].reshape(modes, LANES)
        im = times_i(m)
        turn[0] = m * start_cos[...] + im * start_sin[...]
        turn[1] = im * start_cos[...] - m * start_sin[...]

    load_turn(mg)
    acc[...] = jnp.zeros_like(acc)

    def second(j, carry):
        mode_rhs(turn, rhs)
        synthesise(sy_v, rhs, lhs)
        turn_on(turn, step_cos, step_sin)
        tile_copy(g_hbm, g_v, g_sem, j).wait()
        lines = pl.ds(j * ty, ty)
        pairs = 0.0
        for o in range(chans):
            pre = back_to_x(lhs, l_v, o) + loc_v[o, lines].reshape(tile, nx)
            up = g_v[o, lines].reshape(tile, nx) * twice_gelu_slope(pre)
            g_v[o, lines] = up.reshape(ty, zlines, nx)
            pairs += along_x(up, o, xs, wt_v)
        analyse(pairs, an_v, acc, step_cos, step_sin)
        return carry

    lax.fori_loop(0, steps, second, 0)
    part[1] = spectrum(acc, end_cos, end_sin).reshape(owners, ROWS, LANES)
    scatter_start(part.at[1], got2, s2, r2)

    def back(j, carry):
        def cells(k, carry):
            y, z = j * ty + k // per, k % per
            zs = pl.ds(pl.multiple_of(z * step, step), step)
            ups = [g_v[o, y, zs, :] for o in range(chans)]
            for i in range(chans):
                total = ups[0] * (pw[i, 0] * 0.5)
                for o in range(1, chans):
                    total += ups[o] * (pw[i, o] * 0.5)
                loc_v[i, y, zs, :] = total
            return carry

        lax.fori_loop(0, ty * per, cells, 0)
        return carry

    lax.fori_loop(0, steps, back, 0)

    def last():
        hg[pl.ds(me, 1)] = 0.5 * scatter_sum(part.at[1], got2, s2, r2)[None]
        gather_start(hg, sh, rh)

    owner(last)
    gather_wait(ug, su, ru)
    u_ref[...] = ug[...].reshape(modes, LANES)
    scatter_sent(part.at[0], got1, s1, r1)
    gather_sent(mg, sm, rm)
    gather_sent(ug, su, ru)
    scatter_sent(part.at[1], got2, s2, r2)
    gather_wait(hg, sh, rh)
    h_ref[...] = hg[...].reshape(modes, LANES)
    gather_sent(hg, sh, rh)


def lane_of(kind, chan, wave, width):
    return chan // 2 * (LANES // 2) + kind * (LANES // 4) + chan % 2 * width + wave


def adjoint(h, weights, chans, mx):
    lane = lane_ids(h.shape[0])
    wave, quarter = lane % mx, LANES // 4
    is_real = lane % (LANES // 2) < quarter

    def take(value, index):
        return jnp.take_along_axis(value, index, axis=1)

    chan = lane // mx % chans
    hr, hi = take(h, lane_of(0, chan, wave, mx)), take(h, lane_of(1, chan, wave, mx))
    index = lane % quarter // mx * (LANES // 2) + (chans - 1) * mx + wave
    result = jnp.zeros_like(h)
    for pair in range(2):
        wr, wi = weights[pair], weights[2 + pair]
        for k, value in enumerate((wr * hr + wi * hi, wr * hi - wi * hr)):
            total = value
            for o in range(1, chans):
                total += pltpu.roll(value, o * mx, 1)
            here = (is_real if k == 0 else jnp.logical_not(is_real)) & (lane // (LANES // 2) == pair)
            result = jnp.where(here, take(total, index), result)
    return result


def gradient_kernel(dims, cells_all, u_ref, h_ref, wd_ref, ph_ref, loc_ref, l_ref, sy_ref,
                    o_ref, gs_ref, lhs, turn, rhs, phase, ut, ht):
    chans, mx, my, mz, ylines, zlines, nx, ty, count, cols, owners = dims
    modes = my * mz
    steps = ylines // ty
    j = pl.program_id(0)
    me = lax.axis_index("row") * cols + lax.axis_index("col")

    @pl.when(j == 0)
    def _():
        place = lax.broadcasted_iota(jnp.int32, (modes, count), 1) == me
        found = []
        for k in range(2):
            column = jnp.sum(jnp.where(place, ph_ref[:, k * count : (k + 1) * count], 0.0), axis=1, keepdims=True)
            found.append(jnp.broadcast_to(column, (modes, LANES)))
            phase[k] = jnp.broadcast_to(ph_ref[:, 4 * count + k : 4 * count + k + 1], (modes, LANES))
        m = adjoint(h_ref[...], [wd_ref[b] for b in range(chans)], chans, mx) * (1.0 / HALF_ROOT)
        im = times_i(m)
        turn[0] = m * found[0] + im * found[1]
        turn[1] = im * found[0] - m * found[1]
        ut[...] = u_ref[...].T
        ht[...] = h_ref[...].T

    mode_rhs(turn, rhs)
    synthesise(sy_ref, rhs, lhs)
    turn_on(turn, phase.at[0], phase.at[1])
    blocks = 2 * chans * chans // steps
    wave = lax.broadcasted_iota(jnp.int32, (mx, modes), 0)
    factor = jnp.where(wave == 0, 1.0 / cells_all, 2.0 / cells_all).astype(f32)

    def weight(b):
        at = j * blocks + b
        k, i, o = at // (chans * chans), at // chans % chans, at % chans

        def rows_of(ref, kind, c):
            row = (c // 2 * 4 + kind * 2 + c % 2) * mx
            return ref[pl.ds(pl.multiple_of(row, mx), mx), :]

        ur, ui, hr, hi = rows_of(ut, 0, i), rows_of(ut, 1, i), rows_of(ht, 0, o), rows_of(ht, 1, o)
        value = jnp.where(k == 0, ur * hr + ui * hi, ur * hi - ui * hr) * factor
        for q in range(my):
            lo = q * mz // LANES * LANES
            shift = q * mz - lo
            half = value[:, lo : lo + LANES]
            moved = pltpu.roll(half, LANES - shift, 1) if shift else half
            gs_ref[b * mx : (b + 1) * mx, q, :] = moved[:, :mz]

    share = -(-blocks // chans)
    for i in range(chans):
        out = back_to_x(lhs, l_ref, i)
        o_ref[0, i] = loc_ref[0, i, pl.ds(j * ty, ty)] + out.reshape(ty, zlines, nx)
        for b in range(i * share, min((i + 1) * share, blocks)):
            weight(b)


def solution(mesh):
    nrow, ncol = mesh.shape["row"], mesh.shape["col"]
    count = nrow * ncol

    def per_device(fields, cotangent, spec_weights, point_weights, bias):
        _, chans, ylines, zlines, nx = fields.shape
        _, _, _, mx, my, mz = spec_weights.shape
        ny, nz = ylines * nrow, zlines * ncol
        modes = my * mz
        owners = min(count, modes // ROWS)
        cells_all = float(nx * ny * nz)
        ty = max(1, min(ylines, TILE // zlines))
        steps = ylines // ty
        tile = ty * zlines
        dims = (chans, mx, my, mz, ylines, zlines, nx, ty, count, ncol, owners)
        wt_tab, l_tab = x_tables(chans, nx, mx, cells_all)
        an_tab, sy_tab, ph_tab = yz_tables(ny, nz, my, mz, ty, ylines, zlines, nrow, ncol)
        flat = (2 * chans * chans * mx, my, mz)
        weights = spec_weights.reshape(flat)

        anyspace = pl.BlockSpec(memory_space=pl.ANY)
        vmem = pl.BlockSpec(memory_space=pltpu.VMEM)
        smem = pl.BlockSpec(memory_space=pltpu.SMEM)
        field_shape = jax.ShapeDtypeStruct(fields.shape, f32)
        mode_shape = jax.ShapeDtypeStruct((modes, LANES), f32)
        block = fields.shape[1:]
        gathered = pltpu.VMEM((owners, ROWS, LANES), f32)
        arrived = pltpu.VMEM((count, ROWS, LANES), f32)
        tables = [
            pltpu.VMEM((2 * chans * nx, 2 * LANES), bf16),
            pltpu.VMEM((2 * LANES, 2 * nx), bf16),
            pltpu.VMEM((2 * modes, 2 * tile), bf16),
            pltpu.VMEM((tile, 4 * modes), bf16),
        ]
        lhs_v = pltpu.VMEM((2, tile, 2 * LANES), bf16)
        turn_v = pltpu.VMEM((2, modes, LANES), f32)
        rhs_v = pltpu.VMEM((2 * modes, 2 * LANES), bf16)
        dma = pltpu.SemaphoreType.DMA

        local, spectrum_u, spectrum_h, wide_w = pl.pallas_call(
            functools.partial(layer_kernel, dims),
            out_shape=(pltpu.VMEM(fields.shape, f32),) + (pltpu.VMEM((modes, LANES), f32),) * 2
            + (pltpu.VMEM((4, modes, LANES), f32),),
            in_specs=[anyspace, anyspace, anyspace, smem, smem, anyspace, anyspace, anyspace, anyspace, vmem],
            out_specs=(vmem, vmem, vmem, vmem),
            scratch_shapes=[
                pltpu.VMEM(block, f32), pltpu.VMEM(block, f32),
                pltpu.VMEM(flat, f32),
                *tables,
                pltpu.VMEM((tile, 2 * chans * nx), bf16), lhs_v,
                pltpu.VMEM((2, modes, LANES), f32), turn_v, rhs_v,
                pltpu.VMEM((6, modes, LANES), f32),
                pltpu.VMEM((2, owners, ROWS, LANES), f32),
                arrived, arrived, gathered, gathered, gathered,
                dma((steps,)), dma((steps,)), dma((5,)),
                *[dma((count,))] * 10,
            ],
            compiler_params=pltpu.CompilerParams(
                collective_id=0, has_side_effects=True, vmem_limit_bytes=46 * 1024 * 1024),
            name="layer",
        )(*[pltpu.with_memory_space_constraint(x, pltpu.HBM) for x in (fields, cotangent, weights)],
          point_weights, bias,
          *[pltpu.with_memory_space_constraint(jnp.asarray(x), pltpu.HBM) for x in (wt_tab, l_tab, an_tab, sy_tab)], ph_tab)

        def keep(shape):
            return pl.BlockSpec(shape, lambda j: (0,) * len(shape))

        cells = pl.BlockSpec((1, chans, ty, zlines, nx), lambda j: (0, 0, j, 0, 0))
        mode = keep((modes, LANES))
        grad_fields, grad_spectral = pl.pallas_call(
            functools.partial(gradient_kernel, dims, cells_all),
            grid=(steps,),
            out_shape=(field_shape, jax.ShapeDtypeStruct(flat, f32)),
            in_specs=[mode, mode, keep((4, modes, LANES)), keep(ph_tab.shape), vmem, keep(l_tab.shape), keep(sy_tab.shape)],
            out_specs=(cells, pl.BlockSpec((flat[0] // steps, my, mz), lambda j: (j, 0, 0))),
            scratch_shapes=[
                lhs_v, turn_v, rhs_v, pltpu.VMEM((2, modes, LANES), f32),
                pltpu.VMEM((LANES, modes), f32), pltpu.VMEM((LANES, modes), f32),
            ],
            compiler_params=pltpu.CompilerParams(
                dimension_semantics=("arbitrary",), vmem_limit_bytes=36 * 1024 * 1024),
            name="gradients",
        )(spectrum_u, spectrum_h, wide_w, ph_tab, local, l_tab, sy_tab)
        return grad_fields, grad_spectral.reshape(spec_weights.shape)

    placed = (P(None, None, "row", "col", None), P(None, None, "row", "col", None), P(), P(), P())
    return jax.shard_map(
        per_device,
        mesh=mesh,
        in_specs=placed,
        out_specs=(P(None, None, "row", "col", None), P()),
        check_vma=False,
    )
```

```python
import functools
import math

import jax
import jax.numpy as jnp
import numpy as np
from jax import lax
from jax.experimental import pallas as pl
from jax.experimental.pallas import tpu as pltpu
from jax.sharding import PartitionSpec as P

f32 = jnp.float32
bf16 = jnp.bfloat16
MESH = pl.DeviceIdType.MESH
TILE = 512
ROWS = 8
LANES = 128
HALF_ROOT = math.sqrt(0.5)


def split(value):
    high = value.astype(bf16)
    return high, (value - high.astype(f32)).astype(bf16)


def split_np(value):
    value = np.asarray(value, np.float32)
    high = value.astype(jnp.bfloat16)
    low = (value - high.astype(np.float32)).astype(jnp.bfloat16)
    return high, low


def signed(number):
    wave = np.arange(number)
    return np.where(wave < number // 2, wave, wave - number)


def x_tables(chans, length, modes, cells):
    angle = 2.0 * np.pi / length * ((np.arange(length)[:, None] * np.arange(modes)) % length)
    weight = np.where(np.arange(modes) == 0, 1.0, 2.0) / cells * HALF_ROOT
    first = np.stack([np.cos(angle), -np.sin(angle)], 1)
    eye = np.eye(chans).reshape(chans, chans // 2, 2)
    wide = np.einsum("cgd,xkp->cxgkdp", eye, first).reshape(chans, 1, length, -1)
    wide = np.repeat(wide, 2, 1).reshape(2 * chans * length, -1)
    tall = np.einsum("de,xkp->kdpex", np.eye(2), first * weight).reshape(-1, 2 * length)
    high, low = split_np(tall)
    return np.concatenate(split_np(wide), 1), np.concatenate([high, high, low, 0 * low], 0)


def yz_tables(ny, nz, my, mz, ty, ylines, zlines, nrow, ncol):
    ky, kz = np.repeat(signed(my), mz), np.tile(signed(mz), my)

    def turns(y, z):
        return ((np.outer(y, ky) % ny) / ny + (np.outer(z, kz) % nz) / nz) * 2.0 * np.pi

    angle = turns(np.repeat(np.arange(ty), zlines), np.tile(np.arange(zlines), ty))
    high, low = split_np(np.concatenate([np.cos(angle), np.sin(angle)], 1))
    device_y = np.repeat(np.arange(nrow) * ylines, ncol)
    device_z = np.tile(np.arange(ncol) * zlines, nrow)
    start = turns(device_y, device_z).T
    end = turns(device_y + ylines - ty, device_z).T
    step = turns(np.array([ty]), np.array([0])).T
    phase = np.concatenate(
        [np.cos(start), np.sin(start), np.cos(end), np.sin(end), np.cos(step), np.sin(step)], 1)
    return (np.concatenate([high.T, low.T], 1), np.concatenate([high, low], 1),
            phase.astype(np.float32))


def dot(a, b):
    return jnp.dot(a, b, preferred_element_type=f32)


def lane_ids(rows):
    return lax.broadcasted_iota(jnp.int32, (rows, LANES), 1)


def times_i(value):
    quarter = LANES // 4
    real = lane_ids(value.shape[0]) % (LANES // 2) < quarter
    return jnp.where(real, -pltpu.roll(value, LANES - quarter, 1), pltpu.roll(value, quarter, 1))


def keep_split(value, c, xs):
    width = value.shape[1]
    at = 2 * c * width
    high, low = split(value)
    xs[:, at : at + width] = high
    xs[:, at + width : at + 2 * width] = low


def analyse(pairs, an_v, acc, step_cos, step_sin):
    part = jnp.concatenate(split(pairs[:, :LANES] + pairs[:, LANES:]), 1)
    both = dot(an_v[...], jnp.concatenate([part, part], 0))
    both = both[:, :LANES] + both[:, LANES:]
    modes = both.shape[0] // 2
    c, s = acc[0], acc[1]
    new_c = c * step_cos[...] + s * step_sin[...] + both[:modes]
    new_s = s * step_cos[...] - c * step_sin[...] + both[modes:]
    acc[0] = new_c
    acc[1] = new_s


def spectrum(acc, end_cos, end_sin):
    c, s = acc[0], acc[1]
    cosine = c * end_cos[...] - s * end_sin[...]
    sine = s * end_cos[...] + c * end_sin[...]
    return cosine - times_i(sine)


def mode_rhs(turn, rhs):
    modes = turn.shape[1]
    for k in range(2):
        high, low = split(turn[k])
        rhs[k * modes : (k + 1) * modes, :LANES] = high
        rhs[k * modes : (k + 1) * modes, LANES:] = low


def turn_on(turn, step_cos, step_sin):
    m, im = turn[0], turn[1]
    turn[0] = m * step_cos[...] + im * step_sin[...]
    turn[1] = im * step_cos[...] - m * step_sin[...]


def synthesise(sy_v, rhs, lhs):
    pairs = dot(sy_v[...], jnp.concatenate([rhs[...], rhs[...]], 0))
    value = pairs[:, :LANES] + pairs[:, LANES:]
    other = pltpu.roll(value, LANES // 2, 1)
    lower = lane_ids(value.shape[0]) < LANES // 2
    for pair in range(2):
        twice = jnp.where(lower, value, other) if pair == 0 else jnp.where(lower, other, value)
        high = twice.astype(bf16)
        wide = high.astype(f32)
        lhs[pair, :, :LANES] = jnp.where(lower, wide, twice - wide).astype(bf16)
        lhs[pair, :, LANES:] = high


def back_to_x(lhs, l_v, c):
    nx = l_v.shape[1] // 2
    return dot(lhs[c // 2], l_v[:, c % 2 * nx : (c % 2 + 1) * nx])


def twice_gelu_slope(t):
    gauss = jnp.exp2(t * t * (-1.0 / math.log(2.0)))
    return (lax.erf(t) + 1.0) + (t * (2.0 / math.sqrt(math.pi))) * gauss


def layer_kernel(dims, f_hbm, g_hbm, w_hbm, pw, bias, wt_hbm, l_hbm, an_hbm, sy_hbm, ph_ref,
                 loc_o, u_ref, h_ref, wd_ref,
                 f_v, g_v, w_v, wt_v, l_v, an_v, sy_v, xs, lhs, acc, turn, rhs,
                 phase, part, got1, got2, mg, ug, hg,
                 f_sem, g_sem, tab_sem,
                 s1, r1, sm, rm, su, ru, s2, r2, sh, rh):
    chans, mx, my, mz, ylines, zlines, nx, ty, count, cols, owners = dims
    modes = my * mz
    steps = ylines // ty
    tile = ty * zlines
    loc_v = loc_o.at[0]
    me = lax.axis_index("row") * cols + lax.axis_index("col")

    def device(t):
        return {"row": t // cols, "col": lax.rem(t, cols)}

    barrier = pltpu.get_barrier_semaphore()

    def greet(k, carry):
        pl.semaphore_signal(barrier, inc=1, device_id=device(lax.rem(me + k, count)), device_id_type=MESH)
        return carry

    lax.fori_loop(1, count, greet, 0)

    q = jnp.minimum(me, owners - 1) * ROWS // mz
    r0 = pl.multiple_of(lax.rem(jnp.minimum(me, owners - 1) * ROWS, mz), ROWS)

    def tile_copy(src, dst, sem, j):
        rows = pl.ds(j * ty, ty)
        return pltpu.make_async_copy(src.at[0, :, rows], dst.at[:, rows], sem.at[j])

    wt_copy = pltpu.make_async_copy(wt_hbm, wt_v, tab_sem.at[0])
    l_copy = pltpu.make_async_copy(l_hbm, l_v, tab_sem.at[1])
    an_copy = pltpu.make_async_copy(an_hbm, an_v, tab_sem.at[2])
    sy_copy = pltpu.make_async_copy(sy_hbm, sy_v, tab_sem.at[3])
    w_copy = pltpu.make_async_copy(w_hbm, w_v, tab_sem.at[4])
    wt_copy.start()
    tile_copy(f_hbm, f_v, f_sem, 0).start()
    an_copy.start()
    for j in range(1, steps):
        tile_copy(f_hbm, f_v, f_sem, j).start()
    w_copy.start()
    sy_copy.start()
    l_copy.start()
    for j in range(steps):
        tile_copy(g_hbm, g_v, g_sem, j).start()

    place = lax.broadcasted_iota(jnp.int32, (modes, count), 1) == me
    for k in range(4):
        column = jnp.sum(jnp.where(place, ph_ref[:, k * count : (k + 1) * count], 0.0), axis=1, keepdims=True)
        phase[k] = jnp.broadcast_to(column, (modes, LANES))
    for k in range(2):
        phase[4 + k] = jnp.broadcast_to(ph_ref[:, 4 * count + k : 4 * count + k + 1], (modes, LANES))
    start_cos, start_sin, end_cos, end_sin, step_cos, step_sin = [phase.at[k] for k in range(6)]
    acc[...] = jnp.zeros_like(acc)

    wt_copy.wait()
    an_copy.wait()

    def first(j, carry):
        tile_copy(f_hbm, f_v, f_sem, j).wait()

        for c in range(chans):
            keep_split(f_v[c, pl.ds(j * ty, ty)].reshape(tile, nx), c, xs)
        analyse(dot(xs[...], wt_v[...]), an_v, acc, step_cos, step_sin)
        return carry

    lax.fori_loop(0, steps, first, 0)
    part[0] = spectrum(acc, end_cos, end_sin).reshape(owners, ROWS, LANES)
    pl.semaphore_wait(barrier, count - 1)

    def piece(src, dst, send, recv, k, arriving, scatter):
        t = lax.rem(me + k, count)
        slot = t if arriving else me
        return pltpu.make_async_remote_copy(
            src_ref=src.at[t if scatter else me], dst_ref=dst.at[slot], send_sem=send.at[t],
            recv_sem=recv.at[slot], device_id=device(t), device_id_type=MESH)

    def each(action):
        def body(k, carry):
            action(k)
            return carry
        lax.fori_loop(1, count, body, 0)

    def owned(k, action):
        if owners == count:
            action()
        else:
            pl.when(lax.rem(me + k, count) < owners)(action)

    def owner(action):
        if owners == count:
            action()
        else:
            pl.when(me < owners)(action)

    def scatter_start(src, dst, send, recv):
        each(lambda k: owned(k, lambda: piece(src, dst, send, recv, k, False, True).start()))

    def scatter_sent(src, dst, send, recv):
        each(lambda k: owned(k, lambda: piece(src, dst, send, recv, k, False, True).wait_send()))

    def scatter_sum(src, dst, send, recv):
        each(lambda k: piece(src, dst, send, recv, k, True, False).wait_recv())
        dst[pl.ds(me, 1)] = src[pl.ds(me, 1)]
        return jnp.sum(dst[...], axis=0)

    def gather_start(ref, send, recv):
        each(lambda k: piece(ref, ref, send, recv, k, False, False).start())

    def gather_wait(ref, send, recv):
        each(lambda k: owned(k, lambda: piece(ref, ref, send, recv, k, True, False).wait_recv()))

    def gather_sent(ref, send, recv):
        owner(lambda: each(lambda k: piece(ref, ref, send, recv, k, False, False).wait_send()))

    scatter_start(part.at[0], got1, s1, r1)

    w_copy.wait()
    rows_w = chans * mx * 2
    for b in range(w_v.shape[0] // rows_w):
        wd_ref[b, pl.ds(pl.multiple_of(q * mz, mz), mz), :] = w_v[rows_w * b : rows_w * (b + 1), q, :].T

    step = 16
    per = zlines // step

    def local(k, carry):
        y, z = k // per, k % per
        zs = pl.ds(pl.multiple_of(z * step, step), step)
        fields = [f_v[i, y, zs, :] for i in range(chans)]
        for o in range(chans):
            total = fields[0] * (pw[0, o] * HALF_ROOT) + bias[o] * HALF_ROOT
            for i in range(1, chans):
                total += fields[i] * (pw[i, o] * HALF_ROOT)
            loc_v[o, y, zs, :] = total
        return carry

    lax.fori_loop(0, ylines * per, local, 0)

    lane = lane_ids(ROWS)
    quarter = LANES // 4
    is_real = lane % (LANES // 2) < quarter
    wave = lane % mx

    def lane_of(kind, chan):
        return chan // 2 * (LANES // 2) + kind * quarter + chan % 2 * mx + wave

    def take(value, index):
        return jnp.take_along_axis(value, index, axis=1)

    def weights():
        return [wd_ref[b, pl.ds(pl.multiple_of(q * mz + r0, ROWS), ROWS), :] for b in range(chans)]

    def mix_first():
        u = scatter_sum(part.at[0], got1, s1, r1)
        ug[pl.ds(me, 1)] = u[None]
        w = weights()
        real = imag = 0.0
        for pair in range(2):
            chan = 2 * pair + lane // (LANES // 2)
            ur, ui = take(u, lane_of(0, chan)), take(u, lane_of(1, chan))
            wr, wi = w[pair], w[2 + pair]
            real += wr * ur - wi * ui
            imag += wr * ui + wi * ur
        real += pltpu.roll(real, LANES // 2, 1)
        imag += pltpu.roll(imag, LANES // 2, 1)
        source = lane // (LANES // 2) * quarter + lane % quarter
        mg[pl.ds(me, 1)] = jnp.where(is_real, take(real, source), take(imag, source))[None]
        gather_start(mg, sm, rm)

    owner(mix_first)

    def relay(k, carry):
        row = pl.multiple_of(k * mz, mz)
        for b in range(chans):
            wd_ref[b, pl.ds(row, mz), :] = w_v[rows_w * b : rows_w * (b + 1), k, :].T
        return carry

    lax.fori_loop(0, my, relay, 0)
    sy_copy.wait()
    l_copy.wait()
    gather_wait(mg, sm, rm)
    owner(lambda: gather_start(ug, su, ru))

    def load_turn(ref):
        m = ref[...].reshape(modes, LANES)
        im = times_i(m)
        turn[0] = m * start_cos[...] + im * start_sin[...]
        turn[1] = im * start_cos[...] - m * start_sin[...]

    load_turn(mg)
    acc[...] = jnp.zeros_like(acc)

    def second(j, carry):
        mode_rhs(turn, rhs)
        synthesise(sy_v, rhs, lhs)
        turn_on(turn, step_cos, step_sin)
        tile_copy(g_hbm, g_v, g_sem, j).wait()
        lines = pl.ds(j * ty, ty)
        for o in range(chans):
            pre = back_to_x(lhs, l_v, o) + loc_v[o, lines].reshape(tile, nx)
            up = g_v[o, lines].reshape(tile, nx) * twice_gelu_slope(pre)
            g_v[o, lines] = up.reshape(ty, zlines, nx)
            keep_split(up, o, xs)
        analyse(dot(xs[...], wt_v[...]), an_v, acc, step_cos, step_sin)
        return carry

    lax.fori_loop(0, steps, second, 0)
    part[1] = spectrum(acc, end_cos, end_sin).reshape(owners, ROWS, LANES)
    scatter_start(part.at[1], got2, s2, r2)

    def back(j, carry):
        def cells(k, carry):
            y, z = j * ty + k // per, k % per
            zs = pl.ds(pl.multiple_of(z * step, step), step)
            ups = [g_v[o, y, zs, :] for o in range(chans)]
            for i in range(chans):
                total = ups[0] * (pw[i, 0] * 0.5)
                for o in range(1, chans):
                    total += ups[o] * (pw[i, o] * 0.5)
                loc_v[i, y, zs, :] = total
            return carry

        lax.fori_loop(0, ty * per, cells, 0)
        return carry

    lax.fori_loop(0, steps, back, 0)

    def last():
        hg[pl.ds(me, 1)] = 0.5 * scatter_sum(part.at[1], got2, s2, r2)[None]
        gather_start(hg, sh, rh)

    owner(last)
    gather_wait(ug, su, ru)
    u_ref[...] = ug[...].reshape(modes, LANES)
    scatter_sent(part.at[0], got1, s1, r1)
    gather_sent(mg, sm, rm)
    gather_sent(ug, su, ru)
    scatter_sent(part.at[1], got2, s2, r2)
    gather_wait(hg, sh, rh)
    h_ref[...] = hg[...].reshape(modes, LANES)
    gather_sent(hg, sh, rh)


def lane_of(kind, chan, wave, width):
    return chan // 2 * (LANES // 2) + kind * (LANES // 4) + chan % 2 * width + wave


def adjoint(h, weights, chans, mx):
    lane = lane_ids(h.shape[0])
    wave, quarter = lane % mx, LANES // 4
    is_real = lane % (LANES // 2) < quarter

    def take(value, index):
        return jnp.take_along_axis(value, index, axis=1)

    chan = lane // mx % chans
    hr, hi = take(h, lane_of(0, chan, wave, mx)), take(h, lane_of(1, chan, wave, mx))
    index = lane % quarter // mx * (LANES // 2) + (chans - 1) * mx + wave
    result = jnp.zeros_like(h)
    for pair in range(2):
        wr, wi = weights[pair], weights[2 + pair]
        for k, value in enumerate((wr * hr + wi * hi, wr * hi - wi * hr)):
            total = value
            for o in range(1, chans):
                total += pltpu.roll(value, o * mx, 1)
            here = (is_real if k == 0 else jnp.logical_not(is_real)) & (lane // (LANES // 2) == pair)
            result = jnp.where(here, take(total, index), result)
    return result


def gradient_kernel(dims, cells_all, u_ref, h_ref, wd_ref, ph_ref, loc_ref, l_ref, sy_ref,
                    o_ref, gs_ref, lhs, turn, rhs, phase, ut, ht):
    chans, mx, my, mz, ylines, zlines, nx, ty, count, cols, owners = dims
    modes = my * mz
    steps = ylines // ty
    j = pl.program_id(0)
    me = lax.axis_index("row") * cols + lax.axis_index("col")

    @pl.when(j == 0)
    def _():
        place = lax.broadcasted_iota(jnp.int32, (modes, count), 1) == me
        found = []
        for k in range(2):
            column = jnp.sum(jnp.where(place, ph_ref[:, k * count : (k + 1) * count], 0.0), axis=1, keepdims=True)
            found.append(jnp.broadcast_to(column, (modes, LANES)))
            phase[k] = jnp.broadcast_to(ph_ref[:, 4 * count + k : 4 * count + k + 1], (modes, LANES))
        m = adjoint(h_ref[...], [wd_ref[b] for b in range(chans)], chans, mx) * (1.0 / HALF_ROOT)
        im = times_i(m)
        turn[0] = m * found[0] + im * found[1]
        turn[1] = im * found[0] - m * found[1]
        ut[...] = u_ref[...].T
        ht[...] = h_ref[...].T

    mode_rhs(turn, rhs)
    synthesise(sy_ref, rhs, lhs)
    turn_on(turn, phase.at[0], phase.at[1])
    blocks = 2 * chans * chans // steps
    wave = lax.broadcasted_iota(jnp.int32, (mx, modes), 0)
    factor = jnp.where(wave == 0, 1.0 / cells_all, 2.0 / cells_all).astype(f32)

    def weight(b):
        at = j * blocks + b
        k, i, o = at // (chans * chans), at // chans % chans, at % chans

        def rows_of(ref, kind, c):
            row = (c // 2 * 4 + kind * 2 + c % 2) * mx
            return ref[pl.ds(pl.multiple_of(row, mx), mx), :]

        ur, ui, hr, hi = rows_of(ut, 0, i), rows_of(ut, 1, i), rows_of(ht, 0, o), rows_of(ht, 1, o)
        value = jnp.where(k == 0, ur * hr + ui * hi, ur * hi - ui * hr) * factor
        for q in range(my):
            lo = q * mz // LANES * LANES
            shift = q * mz - lo
            half = value[:, lo : lo + LANES]
            moved = pltpu.roll(half, LANES - shift, 1) if shift else half
            gs_ref[b * mx : (b + 1) * mx, q, :] = moved[:, :mz]

    share = -(-blocks // chans)
    for i in range(chans):
        out = back_to_x(lhs, l_ref, i)
        o_ref[0, i] = loc_ref[0, i, pl.ds(j * ty, ty)] + out.reshape(ty, zlines, nx)
        for b in range(i * share, min((i + 1) * share, blocks)):
            weight(b)


def solution(mesh):
    nrow, ncol = mesh.shape["row"], mesh.shape["col"]
    count = nrow * ncol

    def per_device(fields, cotangent, spec_weights, point_weights, bias):
        _, chans, ylines, zlines, nx = fields.shape
        _, _, _, mx, my, mz = spec_weights.shape
        ny, nz = ylines * nrow, zlines * ncol
        modes = my * mz
        owners = min(count, modes // ROWS)
        cells_all = float(nx * ny * nz)
        ty = max(1, min(ylines, TILE // zlines))
        steps = ylines // ty
        tile = ty * zlines
        dims = (chans, mx, my, mz, ylines, zlines, nx, ty, count, ncol, owners)
        wt_tab, l_tab = x_tables(chans, nx, mx, cells_all)
        an_tab, sy_tab, ph_tab = yz_tables(ny, nz, my, mz, ty, ylines, zlines, nrow, ncol)
        flat = (2 * chans * chans * mx, my, mz)
        weights = spec_weights.reshape(flat)

        anyspace = pl.BlockSpec(memory_space=pl.ANY)
        vmem = pl.BlockSpec(memory_space=pltpu.VMEM)
        smem = pl.BlockSpec(memory_space=pltpu.SMEM)
        field_shape = jax.ShapeDtypeStruct(fields.shape, f32)
        mode_shape = jax.ShapeDtypeStruct((modes, LANES), f32)
        block = fields.shape[1:]
        gathered = pltpu.VMEM((owners, ROWS, LANES), f32)
        arrived = pltpu.VMEM((count, ROWS, LANES), f32)
        tables = [
            pltpu.VMEM((2 * chans * nx, 2 * LANES), bf16),
            pltpu.VMEM((2 * LANES, 2 * nx), bf16),
            pltpu.VMEM((2 * modes, 2 * tile), bf16),
            pltpu.VMEM((tile, 4 * modes), bf16),
        ]
        lhs_v = pltpu.VMEM((2, tile, 2 * LANES), bf16)
        turn_v = pltpu.VMEM((2, modes, LANES), f32)
        rhs_v = pltpu.VMEM((2 * modes, 2 * LANES), bf16)
        dma = pltpu.SemaphoreType.DMA

        local, spectrum_u, spectrum_h, wide_w = pl.pallas_call(
            functools.partial(layer_kernel, dims),
            out_shape=(pltpu.VMEM(fields.shape, f32),) + (pltpu.VMEM((modes, LANES), f32),) * 2
            + (pltpu.VMEM((4, modes, LANES), f32),),
            in_specs=[anyspace, anyspace, anyspace, smem, smem, anyspace, anyspace, anyspace, anyspace, vmem],
            out_specs=(vmem, vmem, vmem, vmem),
            scratch_shapes=[
                pltpu.VMEM(block, f32), pltpu.VMEM(block, f32),
                pltpu.VMEM(flat, f32),
                *tables,
                pltpu.VMEM((tile, 2 * chans * nx), bf16), lhs_v,
                pltpu.VMEM((2, modes, LANES), f32), turn_v, rhs_v,
                pltpu.VMEM((6, modes, LANES), f32),
                pltpu.VMEM((2, owners, ROWS, LANES), f32),
                arrived, arrived, gathered, gathered, gathered,
                dma((steps,)), dma((steps,)), dma((5,)),
                *[dma((count,))] * 10,
            ],
            compiler_params=pltpu.CompilerParams(
                collective_id=0, has_side_effects=True, vmem_limit_bytes=46 * 1024 * 1024),
            name="layer",
        )(*[pltpu.with_memory_space_constraint(x, pltpu.HBM) for x in (fields, cotangent, weights)],
          point_weights, bias,
          *[pltpu.with_memory_space_constraint(jnp.asarray(x), pltpu.HBM) for x in (wt_tab, l_tab, an_tab, sy_tab)], ph_tab)

        def keep(shape):
            return pl.BlockSpec(shape, lambda j: (0,) * len(shape))

        cells = pl.BlockSpec((1, chans, ty, zlines, nx), lambda j: (0, 0, j, 0, 0))
        mode = keep((modes, LANES))
        grad_fields, grad_spectral = pl.pallas_call(
            functools.partial(gradient_kernel, dims, cells_all),
            grid=(steps,),
            out_shape=(field_shape, jax.ShapeDtypeStruct(flat, f32)),
            in_specs=[mode, mode, keep((4, modes, LANES)), keep(ph_tab.shape), vmem, keep(l_tab.shape), keep(sy_tab.shape)],
            out_specs=(cells, pl.BlockSpec((flat[0] // steps, my, mz), lambda j: (j, 0, 0))),
            scratch_shapes=[
                lhs_v, turn_v, rhs_v, pltpu.VMEM((2, modes, LANES), f32),
                pltpu.VMEM((LANES, modes), f32), pltpu.VMEM((LANES, modes), f32),
            ],
            compiler_params=pltpu.CompilerParams(
                dimension_semantics=("arbitrary",), vmem_limit_bytes=36 * 1024 * 1024),
            name="gradients",
        )(spectrum_u, spectrum_h, wide_w, ph_tab, local, l_tab, sy_tab)
        return grad_fields, grad_spectral.reshape(spec_weights.shape)

    placed = (P(None, None, "row", "col", None), P(None, None, "row", "col", None), P(), P(), P())
    return jax.shard_map(
        per_device,
        mesh=mesh,
        in_specs=placed,
        out_specs=(P(None, None, "row", "col", None), P()),
        check_vma=False,
    )
```
